32 devices in a mesh: head: 8 (over y, x, core), seq: 4 (over z).
Axes of the slice: x: 2, y: 2, z: 4, core: 2. Of those that a mesh axis runs over, the one named last changes fastest.
Arguments:
- query_rows: bfloat16 [512, 16384], P('seq', 'head'), may hold values from -512 to 512
- key_rows: bfloat16 [512, 1024], P('seq'), may hold values from -32 to 32
- value_rows: bfloat16 [512, 1024], P('seq'), may hold values from -6 to 6
- positions: int32 [512], P('seq'), may hold values from 0 to 511, as said below
Outputs:
- attended: bfloat16 [512, 16384], P('seq', 'head')
- hessian: float32 [16384, 16384], P('head', 'seq')
The draws below stay inside these ranges and needn't reach their ends.
Inputs may be any that keep to these rules, and one draw needn't show every extreme that they name: Each aligned block of 4 spans of 128 tokens is one sequence; each span holds 128 consecutive ascending positions starting at a multiple of 128, and the sequence's spans together hold every position 0 to 511 once.
All inputs are finite; a program needn't handle non-finite values.
Results may differ from the reference program's by a relative error of at most 0.0037.
Values may be sent and summed in bfloat16 or wider, within the bound.
A program may use at most 128 MiB of HBM per device.

```python
import jax
import jax.numpy as jnp
from jax import lax

HEADS = 128
KVH = 8
HD = 128
TOK_DEV = 128
SPANS = 4
LENGTH = 512
TOKENS = 512


def draw_key_rows(key, part):
    noise_key = jax.random.fold_in(key, 1)
    drawn = jnp.clip(jax.random.normal(noise_key, (TOKENS, KVH * HD), jnp.float32), -4.0, 4.0)
    return drawn.astype(jnp.bfloat16)


def draw_query_rows(key, part):
    noise_key = jax.random.fold_in(key, 2)
    drawn = jnp.clip(jax.random.normal(noise_key, (TOKENS, HEADS * HD), jnp.float32), -4.0, 4.0)
    return drawn.astype(jnp.bfloat16)


def draw_positions(key, part):
    sequence_keys = jax.random.split(jax.random.fold_in(key, 5), TOKENS // LENGTH)
    slots = jax.vmap(lambda single: jax.random.permutation(single, SPANS))(sequence_keys)
    within = jnp.arange(TOK_DEV, dtype=jnp.int32)
    return (slots[:, :, None].astype(jnp.int32) * TOK_DEV + within[None, None, :]).reshape(TOKENS)


def shard_levels(own_key, shape, shards, least, largest):
    level = 1.0
    for position, shards_of in shards:
        steps = jax.random.uniform(jax.random.fold_in(jax.random.fold_in(own_key, 6), position), (shards_of,), jnp.float32, least / len(shards), largest / len(shards))
        level = level * jnp.repeat(jnp.exp(steps), shape[position] // shards_of).reshape((-1,) + (1,) * (len(shape) - 1 - position))
    return level


def noise(rng, dims, spread, limit, cuts=(), kind=jnp.bfloat16):
    entries = jax.random.normal(rng, dims, jnp.float32) * spread
    if len(cuts) > 0:
        entries = shard_levels(rng, dims, cuts, -0.22, 0.18) * entries
    return jnp.clip(entries, min=-limit, max=limit).astype(kind)


def setup_inputs(seed: int = 0) -> dict:
    splits = jax.random.split(jax.random.key(seed), 5)
    query_rows = draw_query_rows(jax.random.fold_in(splits[4], 71), 0)
    key_rows = draw_key_rows(jax.random.fold_in(splits[4], 71), 0)
    value_rows = noise(splits[2], (TOKENS, KVH * HD), 1.0, 6.0, ((0, 4),))
    positions = draw_positions(jax.random.fold_in(splits[4], 71), 0)
    return {"query_rows": query_rows, "key_rows": key_rows, "value_rows": value_rows, "positions": positions}


def reference(query_rows, key_rows, value_rows, positions):
    group_size = HEADS // KVH
    sequence_count = TOKENS // LENGTH
    score_scale = HD ** -0.5
    queries = query_rows.reshape(sequence_count, LENGTH, KVH, group_size, HD)
    queries = jnp.transpose(queries, (0, 2, 3, 1, 4)).reshape(sequence_count, KVH, group_size * LENGTH, HD)
    key_heads = jnp.transpose(key_rows.reshape(sequence_count, LENGTH, KVH, HD), (0, 2, 1, 3))
    value_heads = jnp.transpose(value_rows.reshape(sequence_count, LENGTH, KVH, HD), (0, 2, 1, 3))
    places = positions.reshape(sequence_count, LENGTH)

    def head_group(inputs):
        query_block, key_block, value_block, visible = inputs
        scores = jnp.dot(query_block, key_block.T, preferred_element_type=jnp.float32) * score_scale
        scores = scores.reshape(group_size, LENGTH, LENGTH)
        masked = jnp.where(visible[None], scores, -jnp.inf)
        row_top = jnp.max(masked, axis=2, keepdims=True)
        weights = jnp.exp(masked - row_top)
        weight_sum = jnp.sum(weights, axis=2, keepdims=True)
        mixed = jnp.dot(weights.astype(jnp.bfloat16).reshape(group_size * LENGTH, LENGTH), value_block,
                        preferred_element_type=jnp.float32)
        return (mixed.reshape(group_size, LENGTH, HD) / weight_sum).astype(jnp.bfloat16)

    def sequence_part(inputs):
        query_seq, key_seq, value_seq, place_seq = inputs
        visible = place_seq[None, :] <= place_seq[:, None]
        visible_all = jnp.broadcast_to(visible, (KVH, LENGTH, LENGTH))
        return lax.map(head_group, (query_seq, key_seq, value_seq, visible_all))

    outputs = lax.map(sequence_part, (queries, key_heads, value_heads, places))
    attended = jnp.transpose(outputs, (0, 3, 1, 2, 4)).reshape(TOKENS, HEADS * HD)
    hessian = jnp.dot(attended.T, attended, preferred_element_type=jnp.float32)
    return attended, hessian
```

```python
import functools

import jax
import jax.numpy as jnp
from jax import lax
from jax.experimental import pallas as pl
from jax.experimental.pallas import tpu as pltpu
from jax.sharding import PartitionSpec as P

HEADS = 128
KVH = 8
HD = 128
SPANS = 4
CHUNK_HEADS = 2
TREE_PARTS = 2
LAG = 2
TILE = 512
SLOTS = 4
VMEM_BYTES = 28 * 1024 * 1024
MESH = pl.DeviceIdType.MESH


def exchange_kernel(
    seq_devices, head_devices, chunks,
    q_ref, k_ref, v_ref, pos_ref, attended_ref, turned_ref, cols_ref,
    rows_ref, kbuf, vbuf, pbuf,
    kv_send, kv_recv, line_send, line_recv, tree_send, tree_recv, lane_send, lane_recv,
):
    tokens, width = q_ref.shape
    lanes = head_devices // seq_devices
    bits = seq_devices.bit_length() - 1
    chunk_width = width // chunks
    chunk_heads = chunk_width // HD
    score_scale = HD ** (-0.5)
    head = lax.axis_index("head")
    span = lax.axis_index("seq")
    node, lane = head // lanes, head % lanes
    group = (span // SPANS) * SPANS
    place = span % SPANS

    def flip(bit):
        has = (node // 2**bit) % 2
        return (node + (1 - 2 * has) * 2**bit) * lanes + lane

    far = [(node // 2**bit + span // 2**bit) % 2 for bit in range(bits)]
    above = [sum(far[bit:]) for bit in range(bits)]
    below = [sum(far[: bit + 1]) for bit in range(bits)]
    root = above[0] == 0
    not_root = above[0] > 0

    def peer(step):
        return group + (place + step) % SPANS

    def mate(step):
        return node * lanes + (lane + step) % lanes

    barrier = pltpu.get_barrier_semaphore()
    count = 0
    for step in range(1, SPANS):
        pl.semaphore_signal(barrier, inc=1, device_id={"seq": peer(step)}, device_id_type=MESH)
        count += 1
    for bit in range(bits):
        pl.semaphore_signal(barrier, inc=1, device_id={"head": flip(bit)}, device_id_type=MESH)
        count += 1
    for step in range(1, lanes):
        pl.semaphore_signal(barrier, inc=1, device_id={"head": mate(step)}, device_id_type=MESH)
        count += 1
    if seq_devices > SPANS:
        @pl.when(span > 0)
        def _():
            pl.semaphore_signal(barrier, inc=1, device_id={"seq": span - 1}, device_id_type=MESH)

        @pl.when(span < seq_devices - 1)
        def _():
            pl.semaphore_signal(barrier, inc=1, device_id={"seq": span + 1}, device_id_type=MESH)

        @pl.when(span > 0)
        def _():
            pl.semaphore_wait(barrier, 1)

        @pl.when(span < seq_devices - 1)
        def _():
            pl.semaphore_wait(barrier, 1)

    pl.semaphore_wait(barrier, count)
    key_head = head * (width // HD) // (HEADS // KVH)
    key_columns = pl.ds(pl.multiple_of(key_head * HD, HD), HD)

    def kv_copies(step):
        copies = []
        for which, (src, dst) in enumerate((
            (k_ref.at[:, key_columns], kbuf.at[place]),
            (v_ref.at[:, key_columns], vbuf.at[place]),
            (pos_ref, pbuf.at[place]),
        )):
            copies.append(pltpu.make_async_remote_copy(
                src_ref=src, dst_ref=dst,
                send_sem=kv_send.at[which, step - 1], recv_sem=kv_recv.at[which, step - 1],
                device_id={"seq": peer(step)}, device_id_type=MESH,
            ))
        return copies

    def kv_arrivals(step):
        source = (place + SPANS - step) % SPANS
        copies = []
        for which, (src, dst) in enumerate((
            (k_ref.at[:, key_columns], kbuf.at[source]),
            (v_ref.at[:, key_columns], vbuf.at[source]),
            (pos_ref, pbuf.at[source]),
        )):
            copies.append(pltpu.make_async_remote_copy(
                src_ref=src, dst_ref=dst,
                send_sem=kv_send.at[which, step - 1], recv_sem=kv_recv.at[which, step - 1],
                device_id={"seq": peer(step)}, device_id_type=MESH,
            ))
        return copies

    for step in range(1, SPANS):
        for copy in kv_copies(step):
            copy.start()
    kbuf[place] = k_ref[:, key_columns]
    vbuf[place] = v_ref[:, key_columns]
    pbuf[place] = pos_ref[...]

    def row_chunk(block, part):
        return (
            pl.ds(pl.multiple_of(block * tokens, tokens), tokens),
            pl.ds(pl.multiple_of(part * chunk_width, chunk_width), chunk_width),
        )

    def col_chunk(of_lane, block, part):
        return (
            pl.ds(pl.multiple_of(block * tokens, tokens), tokens),
            pl.ds(pl.multiple_of(of_lane * width + part * chunk_width, chunk_width), chunk_width),
        )

    def line_copy(way, block, part):
        where = rows_ref.at[row_chunk(block, part)]
        return pltpu.make_async_remote_copy(
            src_ref=where, dst_ref=where,
            send_sem=line_send.at[way, block, part], recv_sem=line_recv.at[block, part],
            device_id={"seq": span + 1 - 2 * way}, device_id_type=MESH,
        )

    def tree_copy(bit, block, part, source):
        return pltpu.make_async_remote_copy(
            src_ref=source, dst_ref=cols_ref.at[col_chunk(lane, block, part)],
            send_sem=tree_send.at[bit, block, part], recv_sem=tree_recv.at[block, part],
            device_id={"head": flip(bit)}, device_id_type=MESH,
        )

    def lane_copy(step, of_lane, block, part, source):
        return pltpu.make_async_remote_copy(
            src_ref=source, dst_ref=cols_ref.at[col_chunk(of_lane, block, part)],
            send_sem=lane_send.at[step - 1, block, part],
            recv_sem=lane_recv.at[step - 1, block, part],
            device_id={"head": mate(step)}, device_id_type=MESH,
        )

    def sends(bit, block, part):
        turn = (block + part) % 2
        count = turn * above[bit] + (1 - turn) * below[bit]
        if bits == 2:
            first, last = far[bit], far[1 - bit]
            corner = (first - last) * (first - last)
            middle = 1 - last * (1 - first)
            starts = turn if bit == 1 else 1 - turn
            walk = starts * corner + (1 - starts) * middle
            early = jnp.where(part < chunks - TREE_PARTS, 1, 0)
            count = early * walk + (1 - early) * count
        return count == 0

    def spread(block, part, source):
        for bit in range(bits):
            @pl.when(sends(bit, block, part))
            def _():
                tree_copy(bit, block, part, source).start()
        for step in range(1, lanes):
            lane_copy(step, lane, block, part, source).start()

    def on_row(block, part, up, down):
        @pl.when(up)
        def _():
            line_copy(0, block, part).start()

        @pl.when(down)
        def _():
            line_copy(1, block, part).start()

        @pl.when(root)
        def _():
            spread(block, part, rows_ref.at[row_chunk(block, part)])
            cols_ref[col_chunk(lane, block, part)] = rows_ref[row_chunk(block, part)]

        turned_ref[
            pl.ds(pl.multiple_of(part * chunk_width, chunk_width), chunk_width),
            pl.ds(pl.multiple_of(block * tokens, tokens), tokens),
        ] = rows_ref[row_chunk(block, part)].T

    has_up = span < seq_devices - 1
    has_down = span > 0

    for step in range(1, SPANS):
        for copy in kv_arrivals(step):
            copy.wait_recv()

    keys = kbuf[...].reshape(SPANS * tokens, HD)
    values = vbuf[...].reshape(SPANS * tokens, HD)
    key_places = jnp.concatenate([pbuf[j] for j in range(SPANS)], axis=1)
    query_places = jnp.broadcast_to(pos_ref[0:1, 0:1], (tokens, 1)) + lax.broadcasted_iota(
        jnp.int32, (tokens, 1), 0
    )
    visible = key_places <= query_places

    def compute(part, carry):
        pieces = []
        for h in range(chunk_heads):
            columns = pl.ds(pl.multiple_of(part * chunk_width + h * HD, HD), HD)
            queries = q_ref[:, columns]
            scores = lax.dot_general(
                queries, keys, (((1,), (1,)), ((), ())), preferred_element_type=jnp.float32
            ) * score_scale
            masked = jnp.where(visible, scores, -jnp.inf)
            row_top = jnp.max(masked, axis=1, keepdims=True)
            weights = jnp.exp(masked - row_top)
            weight_sum = jnp.sum(weights, axis=1, keepdims=True)
            mixed = jnp.dot(
                weights.astype(jnp.bfloat16), values, preferred_element_type=jnp.float32
            )
            pieces.append((mixed / weight_sum).astype(jnp.bfloat16))
        joined = jnp.concatenate(pieces, axis=1)
        rows_ref[row_chunk(span, part)] = joined
        attended_ref[:, pl.ds(pl.multiple_of(part * chunk_width, chunk_width), chunk_width)] = joined

        on_row(span, part, has_up, has_down)
        return carry

    lax.fori_loop(0, chunks, compute, 0)

    if bits == 2:
        depths = [
            far[turn] * (1 + far[1 - turn]) + 3 * (1 - far[turn]) * far[1 - turn]
            for turn in range(2)
        ]
        deepest = 3
    else:
        depths = [above[0], above[0]]
        deepest = bits

    def relay(item, carry):
        reach, part = item // chunks, item % chunks
        inside = jnp.logical_and(reach > 0, reach < seq_devices)

        @pl.when(jnp.logical_and(inside, reach <= span))
        def _():
            block = span - reach
            line_copy(0, block, part).wait_recv()
            on_row(block, part, has_up, False)

        @pl.when(jnp.logical_and(inside, span + reach < seq_devices))
        def _():
            block = span + reach
            line_copy(1, block, part).wait_recv()
            on_row(block, part, False, has_down)

        for turn in range(2):
            late = item - LAG * depths[turn]
            distance, piece = late // chunks, late % chunks
            known = jnp.logical_and(not_root, late >= 0)

            def from_parent(block, piece=piece):
                source = cols_ref.at[col_chunk(lane, block, piece)]
                tree_copy(0, block, piece, source).wait_recv()
                spread(block, piece, source)

            @pl.when(
                jnp.logical_and(
                    jnp.logical_and(known, distance <= span),
                    (span + seq_devices - distance + piece + turn) % 2 == 0,
                )
            )
            def _():
                from_parent(span - distance)

            @pl.when(
                jnp.logical_and(
                    jnp.logical_and(known, distance > 0),
                    jnp.logical_and(
                        span + distance < seq_devices,
                        (span + distance + piece + turn) % 2 == 0,
                    ),
                )
            )
            def _():
                from_parent(span + distance)

        return carry

    lax.fori_loop(0, seq_devices * chunks + LAG * deepest, relay, 0)

    def drain(item, carry):
        block, part = item // chunks, item % chunks
        source = cols_ref.at[col_chunk(lane, block, part)]

        @pl.when(jnp.logical_and(has_up, block <= span))
        def _():
            line_copy(0, block, part).wait_send()

        @pl.when(jnp.logical_and(has_down, block >= span))
        def _():
            line_copy(1, block, part).wait_send()

        for bit in range(bits):
            @pl.when(sends(bit, block, part))
            def _():
                tree_copy(bit, block, part, source).wait_send()
        for step in range(1, lanes):
            lane_copy(step, lane, block, part, source).wait_send()
            lane_copy(step, (lane + lanes - step) % lanes, block, part, source).wait_recv()
        return carry

    lax.fori_loop(0, seq_devices * chunks, drain, 0)

    for step in range(1, SPANS):
        for copy in kv_copies(step):
            copy.wait_send()


def hessian_kernel(own_ref, turned_ref, cols_ref, attended_ref, out_ref, ring, own_sem, ring_sem):
    tile = ring.shape[2]
    slots = ring.shape[0]
    tiles = out_ref.shape[1] // tile
    own = pltpu.make_async_copy(own_ref, attended_ref, own_sem)
    own.start()

    def columns(j):
        return pl.ds(pl.multiple_of(j * tile, tile), tile)

    def put(j):
        slot = j % slots
        return pltpu.make_async_copy(ring.at[slot], out_ref.at[:, columns(j)], ring_sem.at[slot])

    def body(j, carry):
        @pl.when(j >= slots)
        def _():
            put(j - slots).wait()

        ring[j % slots] = jnp.dot(
            turned_ref[...], cols_ref[:, columns(j)], preferred_element_type=jnp.float32
        )
        put(j).start()
        return carry

    lax.fori_loop(0, tiles, body, 0)
    for j in range(max(0, tiles - slots), tiles):
        put(j).wait()
    own.wait()


def on_device(query_rows, key_rows, value_rows, positions):
    tokens, width = query_rows.shape
    seq_devices = lax.axis_size("seq")
    head_devices = lax.axis_size("head")
    lanes = head_devices // seq_devices
    bits = seq_devices.bit_length() - 1
    chunks = max(1, width // (CHUNK_HEADS * HD))
    vmem = pl.BlockSpec(memory_space=pltpu.VMEM)
    dma = pltpu.SemaphoreType.DMA
    own, turned, cols = pl.pallas_call(
        functools.partial(exchange_kernel, seq_devices, head_devices, chunks),
        out_shape=(
            jax.ShapeDtypeStruct((tokens, width), jnp.bfloat16),
            jax.ShapeDtypeStruct((width, seq_devices * tokens), jnp.bfloat16),
            jax.ShapeDtypeStruct((seq_devices * tokens, lanes * width), jnp.bfloat16),
        ),
        in_specs=[vmem] * 4,
        out_specs=(vmem, vmem, vmem),
        scratch_shapes=[
            pltpu.VMEM((seq_devices * tokens, width), jnp.bfloat16),
            pltpu.VMEM((SPANS, tokens, HD), jnp.bfloat16),
            pltpu.VMEM((SPANS, tokens, HD), jnp.bfloat16),
            pltpu.VMEM((SPANS, 1, tokens), jnp.int32),
            dma((3, SPANS - 1)),
            dma((3, SPANS - 1)),
            dma((2, seq_devices, chunks)),
            dma((seq_devices, chunks)),
            dma((bits, seq_devices, chunks)),
            dma((seq_devices, chunks)),
            dma((lanes - 1, seq_devices, chunks)),
            dma((lanes - 1, seq_devices, chunks)),
        ],
        compiler_params=pltpu.CompilerParams(
            collective_id=0, has_side_effects=True, vmem_limit_bytes=VMEM_BYTES
        ),
        name="attend_exchange",
    )(query_rows, key_rows, value_rows, positions.reshape(1, tokens))
    breadth = cols.shape[1]
    tile = min(TILE, breadth)
    slots = min(SLOTS, breadth // tile)
    attended, hessian = pl.pallas_call(
        hessian_kernel,
        out_shape=(
            jax.ShapeDtypeStruct((tokens, width), jnp.bfloat16),
            jax.ShapeDtypeStruct((width, breadth), jnp.float32),
        ),
        in_specs=[vmem] * 3,
        out_specs=(pl.BlockSpec(memory_space=pl.ANY), pl.BlockSpec(memory_space=pl.ANY)),
        scratch_shapes=[
            pltpu.VMEM((slots, width, tile), jnp.float32),
            dma,
            dma((slots,)),
        ],
        compiler_params=pltpu.CompilerParams(vmem_limit_bytes=VMEM_BYTES),
        name="hessian",
    )(own, turned, cols)
    return (attended, hessian)


def solution(mesh):
    placed = (P("seq", "head"), P("seq", None), P("seq", None), P("seq"))
    return jax.shard_map(
        on_device,
        mesh=mesh,
        in_specs=placed,
        out_specs=(P("seq", "head"), P("head", "seq")),
        check_vma=False,
    )
```

```python
import functools

import jax
import jax.numpy as jnp
from jax import lax
from jax.experimental import pallas as pl
from jax.experimental.pallas import tpu as pltpu
from jax.sharding import PartitionSpec as P

HEADS = 128
KVH = 8
HD = 128
SPANS = 4
CHUNK_HEADS = 2
TREE_PARTS = 2
LEAD = 0
LAG = 3
RAW_PARTS = 0
TILE = 512
PIECES = 4
SLOTS = 4
VMEM_BYTES = 28 * 1024 * 1024
MESH = pl.DeviceIdType.MESH


def exchange_kernel(
    seq_devices, head_devices, chunks, raw_parts,
    q_hbm, k_hbm, v_hbm, pos_hbm, attended_ref, turned_ref, cols_ref,
    q_ref, raw_ref, rows_ref, kbuf, vbuf, pbuf,
    load_sems, kv_send, kv_recv, line_send, line_recv, tree_send, tree_recv, lane_send, lane_recv,
):
    tokens, width = q_ref.shape
    lanes = head_devices // seq_devices
    bits = seq_devices.bit_length() - 1
    chunk_width = width // chunks
    chunk_heads = chunk_width // HD
    raw_width = raw_parts * chunk_width
    score_scale = HD ** (-0.5)
    head = lax.axis_index("head")
    span = lax.axis_index("seq")
    node, lane = head // lanes, head % lanes
    group = (span // SPANS) * SPANS
    place = span % SPANS

    def flip(bit):
        has = (node // 2**bit) % 2
        return (node + (1 - 2 * has) * 2**bit) * lanes + lane

    far = [(node // 2**bit + span // 2**bit) % 2 for bit in range(bits)]
    above = [sum(far[bit:]) for bit in range(bits)]
    below = [sum(far[: bit + 1]) for bit in range(bits)]
    root = above[0] == 0
    not_root = above[0] > 0

    def peer(step):
        return group + (place + step) % SPANS

    def mate(step):
        return node * lanes + (lane + step) % lanes

    key_head = head * (width // HD) // (HEADS // KVH)
    key_columns = pl.ds(pl.multiple_of(key_head * HD, HD), HD)
    own_rows = pl.ds(pl.multiple_of(span * tokens, tokens), tokens)
    loads = [
        pltpu.make_async_copy(k_hbm.at[:, key_columns], kbuf.at[place], load_sems.at[0]),
        pltpu.make_async_copy(v_hbm.at[:, key_columns], vbuf.at[place], load_sems.at[1]),
        pltpu.make_async_copy(pos_hbm, pbuf.at[place], load_sems.at[2]),
        pltpu.make_async_copy(q_hbm, q_ref, load_sems.at[3]),
    ]
    if raw_parts:
        loads.append(
            pltpu.make_async_copy(
                q_hbm.at[:, pl.ds(0, raw_width)], raw_ref.at[own_rows], load_sems.at[4]
            )
        )
    for load in loads:
        load.start()

    barrier = pltpu.get_barrier_semaphore()
    count = 0
    for step in range(1, SPANS):
        pl.semaphore_signal(barrier, inc=1, device_id={"seq": peer(step)}, device_id_type=MESH)
        count += 1
    for bit in range(bits):
        pl.semaphore_signal(barrier, inc=1, device_id={"head": flip(bit)}, device_id_type=MESH)
        count += 1
    for step in range(1, lanes):
        pl.semaphore_signal(barrier, inc=1, device_id={"head": mate(step)}, device_id_type=MESH)
        count += 1
    if seq_devices > SPANS:
        @pl.when(span > 0)
        def _():
            pl.semaphore_signal(barrier, inc=1, device_id={"seq": span - 1}, device_id_type=MESH)

        @pl.when(span < seq_devices - 1)
        def _():
            pl.semaphore_signal(barrier, inc=1, device_id={"seq": span + 1}, device_id_type=MESH)

        @pl.when(span > 0)
        def _():
            pl.semaphore_wait(barrier, 1)

        @pl.when(span < seq_devices - 1)
        def _():
            pl.semaphore_wait(barrier, 1)

    for load in loads:
        load.wait()
    pl.semaphore_wait(barrier, count)

    def kv_copies(step):
        copies = []
        for which, (src, dst) in enumerate((
            (kbuf.at[place], kbuf.at[place]),
            (vbuf.at[place], vbuf.at[place]),
            (pbuf.at[place], pbuf.at[place]),
        )):
            copies.append(pltpu.make_async_remote_copy(
                src_ref=src, dst_ref=dst,
                send_sem=kv_send.at[which, step - 1], recv_sem=kv_recv.at[which, step - 1],
                device_id={"seq": peer(step)}, device_id_type=MESH,
            ))
        return copies

    def kv_arrivals(step):
        source = (place + SPANS - step) % SPANS
        copies = []
        for which, (src, dst) in enumerate((
            (kbuf.at[source], kbuf.at[source]),
            (vbuf.at[source], vbuf.at[source]),
            (pbuf.at[source], pbuf.at[source]),
        )):
            copies.append(pltpu.make_async_remote_copy(
                src_ref=src, dst_ref=dst,
                send_sem=kv_send.at[which, step - 1], recv_sem=kv_recv.at[which, step - 1],
                device_id={"seq": peer(step)}, device_id_type=MESH,
            ))
        return copies

    for step in range(1, SPANS):
        for copy in kv_copies(step):
            copy.start()

    def row_chunk(block, part):
        return (
            pl.ds(pl.multiple_of(block * tokens, tokens), tokens),
            pl.ds(pl.multiple_of(part * chunk_width, chunk_width), chunk_width),
        )

    def col_chunk(of_lane, block, part):
        return (
            pl.ds(pl.multiple_of(block * tokens, tokens), tokens),
            pl.ds(pl.multiple_of(of_lane * width + part * chunk_width, chunk_width), chunk_width),
        )

    def line_copy(way, block, part, held=rows_ref):
        where = held.at[row_chunk(block, part)]
        return pltpu.make_async_remote_copy(
            src_ref=where, dst_ref=where,
            send_sem=line_send.at[way, block, part], recv_sem=line_recv.at[block, part],
            device_id={"seq": span + 1 - 2 * way}, device_id_type=MESH,
        )

    def tree_copy(bit, block, part, source):
        return pltpu.make_async_remote_copy(
            src_ref=source, dst_ref=cols_ref.at[col_chunk(lane, block, part)],
            send_sem=tree_send.at[bit, block, part], recv_sem=tree_recv.at[block, part],
            device_id={"head": flip(bit)}, device_id_type=MESH,
        )

    def lane_copy(step, of_lane, block, part, source):
        return pltpu.make_async_remote_copy(
            src_ref=source, dst_ref=cols_ref.at[col_chunk(of_lane, block, part)],
            send_sem=lane_send.at[step - 1, block, part],
            recv_sem=lane_recv.at[step - 1, block, part],
            device_id={"head": mate(step)}, device_id_type=MESH,
        )

    farthest = jnp.maximum(span, seq_devices - 1 - span)

    def walks(block, part):
        final = jnp.logical_and(
            jnp.abs(block - span) == farthest, part >= chunks - TREE_PARTS
        )
        return jnp.where(final, 0, 1)

    def sends(bit, block, part):
        turn = (block + part) % 2
        count = turn * above[bit] + (1 - turn) * below[bit]
        if bits == 2:
            first, last = far[bit], far[1 - bit]
            corner = (first - last) * (first - last)
            middle = 1 - last * (1 - first)
            starts = turn if bit == 1 else 1 - turn
            walk = starts * corner + (1 - starts) * middle
            walked = walks(block, part)
            count = walked * walk + (1 - walked) * count
        return count == 0

    def spread(block, part, source):
        for bit in range(bits):
            @pl.when(sends(bit, block, part))
            def _():
                tree_copy(bit, block, part, source).start()
        for step in range(1, lanes):
            lane_copy(step, lane, block, part, source).start()

    def pass_on(block, part, up, down, held=rows_ref):
        @pl.when(up)
        def _():
            line_copy(0, block, part, held).start()

        @pl.when(down)
        def _():
            line_copy(1, block, part, held).start()

    def on_row(block, part):
        @pl.when(root)
        def _():
            spread(block, part, rows_ref.at[row_chunk(block, part)])
            cols_ref[col_chunk(lane, block, part)] = rows_ref[row_chunk(block, part)]

        turned_ref[
            pl.ds(pl.multiple_of(part * chunk_width, chunk_width), chunk_width),
            pl.ds(pl.multiple_of(block * tokens, tokens), tokens),
        ] = rows_ref[row_chunk(block, part)].T

    has_up = span < seq_devices - 1
    has_down = span > 0

    for part in range(raw_parts):
        pass_on(span, part, has_up, has_down, raw_ref)

    for step in range(1, SPANS):
        for copy in kv_arrivals(step):
            copy.wait_recv()

    keys = kbuf[...].reshape(SPANS * tokens, HD)
    values = vbuf[...].reshape(SPANS * tokens, HD)
    key_places = jnp.concatenate([pbuf[j] for j in range(SPANS)], axis=1)

    def attend(held, rows, part, at):
        query_places = jnp.broadcast_to(pbuf[at][0:1, 0:1], (tokens, 1)) + lax.broadcasted_iota(
            jnp.int32, (tokens, 1), 0
        )
        visible = key_places <= query_places
        pieces = []
        for h in range(chunk_heads):
            columns = pl.ds(pl.multiple_of(part * chunk_width + h * HD, HD), HD)
            queries = held[rows, columns]
            scores = lax.dot_general(
                queries, keys, (((1,), (1,)), ((), ())), preferred_element_type=jnp.float32
            ) * score_scale
            masked = jnp.where(visible, scores, -jnp.inf)
            row_top = jnp.max(masked, axis=1, keepdims=True)
            weights = jnp.exp(masked - row_top)
            weight_sum = jnp.sum(weights, axis=1, keepdims=True)
            mixed = jnp.dot(
                weights.astype(jnp.bfloat16), values, preferred_element_type=jnp.float32
            )
            pieces.append((mixed / weight_sum).astype(jnp.bfloat16))
        return jnp.concatenate(pieces, axis=1)

    def compute(step, carry):
        part = (step + raw_parts) % chunks
        joined = attend(q_ref, pl.ds(0, tokens), part, place)
        rows_ref[row_chunk(span, part)] = joined
        attended_ref[:, pl.ds(pl.multiple_of(part * chunk_width, chunk_width), chunk_width)] = joined
        sent = part >= raw_parts
        pass_on(span, part, jnp.logical_and(has_up, sent), jnp.logical_and(has_down, sent))
        on_row(span, part)
        return carry

    lax.fori_loop(0, chunks, compute, 0)

    def arrive(way, block, part):
        up = has_up if way == 0 else False
        down = has_down if way == 1 else False

        def ready():
            line_copy(way, block, part).wait_recv()
            pass_on(block, part, up, down)

        if raw_parts:
            @pl.when(part >= raw_parts)
            def _():
                ready()

            @pl.when(part < raw_parts)
            def _():
                line_copy(way, block, part, raw_ref).wait_recv()
                pass_on(block, part, up, down, raw_ref)
                rows_ref[row_chunk(block, part)] = attend(
                    raw_ref, pl.ds(pl.multiple_of(block * tokens, tokens), tokens), part,
                    block % SPANS,
                )
        else:
            ready()
        on_row(block, part)

    classes = [(0, False), (1, False)]
    deepest = bits
    if bits == 2:
        classes = [(0, True), (1, True)] + classes
        deepest = 3
        depths = [
            far[turn] * (1 + far[1 - turn]) + 3 * (1 - far[turn]) * far[1 - turn]
            for turn in range(2)
        ]

    def relay(item, carry):
        reach, part = item // chunks, item % chunks
        inside = jnp.logical_and(reach > 0, reach < seq_devices)

        @pl.when(jnp.logical_and(inside, reach <= span))
        def _():
            arrive(0, span - reach, part)

        @pl.when(jnp.logical_and(inside, span + reach < seq_devices))
        def _():
            arrive(1, span + reach, part)

        for turn, walked in classes:
            late = item - LEAD - LAG * (depths[turn] if walked else above[0])
            distance, piece = late // chunks, late % chunks
            known = jnp.logical_and(not_root, late >= 0)

            def mine(block, piece=piece, turn=turn, walked=walked):
                match = (block + seq_devices + piece + turn) % 2 == 0
                if bits == 2:
                    match = jnp.logical_and(match, walks(block, piece) == (1 if walked else 0))
                return match

            def from_parent(block, piece=piece):
                source = cols_ref.at[col_chunk(lane, block, piece)]
                tree_copy(0, block, piece, source).wait_recv()
                spread(block, piece, source)

            @pl.when(
                jnp.logical_and(
                    jnp.logical_and(known, distance <= span), mine(span - distance)
                )
            )
            def _():
                from_parent(span - distance)

            @pl.when(
                jnp.logical_and(
                    jnp.logical_and(known, distance > 0),
                    jnp.logical_and(span + distance < seq_devices, mine(span + distance)),
                )
            )
            def _():
                from_parent(span + distance)

        return carry

    lax.fori_loop(0, seq_devices * chunks + LEAD + LAG * deepest, relay, 0)

    def drain(item, carry):
        block, part = item // chunks, item % chunks
        source = cols_ref.at[col_chunk(lane, block, part)]

        @pl.when(jnp.logical_and(has_up, block <= span))
        def _():
            line_copy(0, block, part).wait_send()

        @pl.when(jnp.logical_and(has_down, block >= span))
        def _():
            line_copy(1, block, part).wait_send()

        for bit in range(bits):
            @pl.when(sends(bit, block, part))
            def _():
                tree_copy(bit, block, part, source).wait_send()
        for step in range(1, lanes):
            lane_copy(step, lane, block, part, source).wait_send()
            lane_copy(step, (lane + lanes - step) % lanes, block, part, source).wait_recv()
        return carry

    lax.fori_loop(0, seq_devices * chunks, drain, 0)

    for step in range(1, SPANS):
        for copy in kv_copies(step):
            copy.wait_send()


def hessian_kernel(own_ref, turned_ref, cols_ref, attended_ref, out_ref, ring, own_sem, ring_sem):
    tile = ring.shape[2]
    slots = ring.shape[0]
    tiles = out_ref.shape[1] // tile
    own = pltpu.make_async_copy(own_ref, attended_ref, own_sem)
    own.start()

    def columns(j):
        return pl.ds(pl.multiple_of(j * tile, tile), tile)

    rows = out_ref.shape[0] // PIECES

    def put(j, piece):
        slot = j % slots
        where = pl.ds(piece * rows, rows)
        return pltpu.make_async_copy(
            ring.at[slot, where], out_ref.at[where, columns(j)], ring_sem.at[slot, piece]
        )

    def body(j, carry):
        @pl.when(j >= slots)
        def _():
            for piece in range(PIECES):
                put(j - slots, piece).wait()

        block = cols_ref[:, columns(j)]
        for piece in range(PIECES):
            where = pl.ds(piece * rows, rows)
            ring[j % slots, where] = jnp.dot(
                turned_ref[where, :], block, preferred_element_type=jnp.float32
            )
            put(j, piece).start()
        return carry

    lax.fori_loop(0, tiles, body, 0)
    for j in range(max(0, tiles - slots), tiles):
        for piece in range(PIECES):
            put(j, piece).wait()
    own.wait()


def on_device(query_rows, key_rows, value_rows, positions):
    tokens, width = query_rows.shape
    seq_devices = lax.axis_size("seq")
    head_devices = lax.axis_size("head")
    lanes = head_devices // seq_devices
    bits = seq_devices.bit_length() - 1
    chunks = max(1, width // (CHUNK_HEADS * HD))
    raw_parts = min(RAW_PARTS, chunks - 1) if seq_devices == SPANS else 0
    vmem = pl.BlockSpec(memory_space=pltpu.VMEM)
    arguments = [
        pltpu.with_memory_space_constraint(array, pltpu.HBM)
        for array in (query_rows, key_rows, value_rows, positions.reshape(1, tokens))
    ]
    dma = pltpu.SemaphoreType.DMA
    own, turned, cols = pl.pallas_call(
        functools.partial(exchange_kernel, seq_devices, head_devices, chunks, raw_parts),
        out_shape=(
            jax.ShapeDtypeStruct((tokens, width), jnp.bfloat16),
            jax.ShapeDtypeStruct((width, seq_devices * tokens), jnp.bfloat16),
            jax.ShapeDtypeStruct((seq_devices * tokens, lanes * width), jnp.bfloat16),
        ),
        in_specs=[pl.BlockSpec(memory_space=pltpu.HBM)] * 4,
        out_specs=(vmem, vmem, vmem),
        scratch_shapes=[
            pltpu.VMEM((tokens, width), jnp.bfloat16),
            pltpu.VMEM(
                (seq_devices * tokens, max(1, raw_parts) * width // chunks), jnp.bfloat16
            ),
            pltpu.VMEM((seq_devices * tokens, width), jnp.bfloat16),
            pltpu.VMEM((SPANS, tokens, HD), jnp.bfloat16),
            pltpu.VMEM((SPANS, tokens, HD), jnp.bfloat16),
            pltpu.VMEM((SPANS, 1, tokens), jnp.int32),
            dma((5,)),
            dma((3, SPANS - 1)),
            dma((3, SPANS - 1)),
            dma((2, seq_devices, chunks)),
            dma((seq_devices, chunks)),
            dma((bits, seq_devices, chunks)),
            dma((seq_devices, chunks)),
            dma((lanes - 1, seq_devices, chunks)),
            dma((lanes - 1, seq_devices, chunks)),
        ],
        compiler_params=pltpu.CompilerParams(
            collective_id=0, has_side_effects=True, vmem_limit_bytes=VMEM_BYTES
        ),
        name="attend_exchange",
    )(*arguments)
    breadth = cols.shape[1]
    tile = min(TILE, breadth)
    slots = min(SLOTS, breadth // tile)
    attended, hessian = pl.pallas_call(
        hessian_kernel,
        out_shape=(
            jax.ShapeDtypeStruct((tokens, width), jnp.bfloat16),
            jax.ShapeDtypeStruct((width, breadth), jnp.float32),
        ),
        in_specs=[vmem] * 3,
        out_specs=(pl.BlockSpec(memory_space=pl.ANY), pl.BlockSpec(memory_space=pl.ANY)),
        scratch_shapes=[
            pltpu.VMEM((slots, width, tile), jnp.float32),
            dma,
            dma((slots, PIECES)),
        ],
        compiler_params=pltpu.CompilerParams(vmem_limit_bytes=VMEM_BYTES),
        name="hessian",
    )(own, turned, cols)
    return (attended, hessian)


def solution(mesh):
    placed = (P("seq", "head"), P("seq", None), P("seq", None), P("seq"))
    return jax.shard_map(
        on_device,
        mesh=mesh,
        in_specs=placed,
        out_specs=(P("seq", "head"), P("head", "seq")),
        check_vma=False,
    )
```

```python
import functools

import jax
import jax.numpy as jnp
from jax import lax
from jax.experimental import pallas as pl
from jax.experimental.pallas import tpu as pltpu
from jax.sharding import PartitionSpec as P

HEADS = 128
KVH = 8
HD = 128
SPANS = 4
CHUNK_HEADS = 2
COMPUTE_HEADS = 4
LEAD = 0
LAG_ONE = 2
LAG_TWO = 3
LAG_THREE = 5
RAW_PAIRS = 1
TILE = 512
PIECES = 4
SLOTS = 4
VMEM_BYTES = 28 * 1024 * 1024
MESH = pl.DeviceIdType.MESH


def exchange_kernel(
    seq_devices, head_devices, chunks, raw_pairs,
    q_hbm, k_hbm, v_hbm, pos_hbm, attended_ref, turned_ref, cols_ref,
    q_ref, raw_ref, rows_ref, kbuf, vbuf, pbuf,
    load_sems, kv_send, kv_recv, line_send, line_recv, tree_send, tree_recv, lane_send, lane_recv,
):
    tokens, width = q_ref.shape
    lanes = head_devices // seq_devices
    bits = seq_devices.bit_length() - 1
    chunk_width = width // chunks
    chunk_heads = chunk_width // HD
    raw_width = raw_pairs * 2 * chunk_width
    score_scale = HD ** (-0.5)
    head = lax.axis_index("head")
    span = lax.axis_index("seq")
    node, lane = head // lanes, head % lanes
    group = (span // SPANS) * SPANS
    place = span % SPANS

    def flip(bit):
        has = (node // 2**bit) % 2
        return (node + (1 - 2 * has) * 2**bit) * lanes + lane

    far = [(node // 2**bit + span // 2**bit) % 2 for bit in range(bits)]
    above = [sum(far[bit:]) for bit in range(bits)]
    below = [sum(far[: bit + 1]) for bit in range(bits)]
    root = above[0] == 0
    not_root = above[0] > 0

    def peer(step):
        return group + (place + step) % SPANS

    def mate(step):
        return node * lanes + (lane + step) % lanes

    key_head = head * (width // HD) // (HEADS // KVH)
    key_columns = pl.ds(pl.multiple_of(key_head * HD, HD), HD)
    own_rows = pl.ds(pl.multiple_of(span * tokens, tokens), tokens)
    loads = [
        pltpu.make_async_copy(k_hbm.at[:, key_columns], kbuf.at[place], load_sems.at[0]),
        pltpu.make_async_copy(v_hbm.at[:, key_columns], vbuf.at[place], load_sems.at[1]),
        pltpu.make_async_copy(pos_hbm, pbuf.at[place], load_sems.at[2]),
        pltpu.make_async_copy(q_hbm, q_ref, load_sems.at[3]),
    ]
    if raw_pairs:
        loads.append(
            pltpu.make_async_copy(
                q_hbm.at[:, pl.ds(0, raw_width)], raw_ref.at[own_rows], load_sems.at[4]
            )
        )
    for load in loads:
        load.start()

    barrier = pltpu.get_barrier_semaphore()
    count = 0
    for step in range(1, SPANS):
        pl.semaphore_signal(barrier, inc=1, device_id={"seq": peer(step)}, device_id_type=MESH)
        count += 1
    for bit in range(bits):
        pl.semaphore_signal(barrier, inc=1, device_id={"head": flip(bit)}, device_id_type=MESH)
        count += 1
    for step in range(1, lanes):
        pl.semaphore_signal(barrier, inc=1, device_id={"head": mate(step)}, device_id_type=MESH)
        count += 1
    if seq_devices > SPANS:
        @pl.when(span > 0)
        def _():
            pl.semaphore_signal(barrier, inc=1, device_id={"seq": span - 1}, device_id_type=MESH)

        @pl.when(span < seq_devices - 1)
        def _():
            pl.semaphore_signal(barrier, inc=1, device_id={"seq": span + 1}, device_id_type=MESH)

        @pl.when(span > 0)
        def _():
            pl.semaphore_wait(barrier, 1)

        @pl.when(span < seq_devices - 1)
        def _():
            pl.semaphore_wait(barrier, 1)

    for load in loads:
        load.wait()
    pl.semaphore_wait(barrier, count)

    def kv_copies(step):
        copies = []
        for which, (src, dst) in enumerate((
            (kbuf.at[place], kbuf.at[place]),
            (vbuf.at[place], vbuf.at[place]),
            (pbuf.at[place], pbuf.at[place]),
        )):
            copies.append(pltpu.make_async_remote_copy(
                src_ref=src, dst_ref=dst,
                send_sem=kv_send.at[which, step - 1], recv_sem=kv_recv.at[which, step - 1],
                device_id={"seq": peer(step)}, device_id_type=MESH,
            ))
        return copies

    def kv_arrivals(step):
        source = (place + SPANS - step) % SPANS
        copies = []
        for which, (src, dst) in enumerate((
            (kbuf.at[source], kbuf.at[source]),
            (vbuf.at[source], vbuf.at[source]),
            (pbuf.at[source], pbuf.at[source]),
        )):
            copies.append(pltpu.make_async_remote_copy(
                src_ref=src, dst_ref=dst,
                send_sem=kv_send.at[which, step - 1], recv_sem=kv_recv.at[which, step - 1],
                device_id={"seq": peer(step)}, device_id_type=MESH,
            ))
        return copies

    for step in range(1, SPANS):
        for copy in kv_copies(step):
            copy.start()

    def row_chunk(block, part):
        return (
            pl.ds(pl.multiple_of(block * tokens, tokens), tokens),
            pl.ds(pl.multiple_of(part * chunk_width, chunk_width), chunk_width),
        )

    def col_chunk(of_lane, block, part):
        return (
            pl.ds(pl.multiple_of(block * tokens, tokens), tokens),
            pl.ds(pl.multiple_of(of_lane * width + part * chunk_width, chunk_width), chunk_width),
        )

    def block_rows(block):
        return pl.ds(pl.multiple_of(block * tokens, tokens), tokens)

    def line_copy(way, block, part, held=rows_ref):
        where = held.at[row_chunk(block, part)]
        return pltpu.make_async_remote_copy(
            src_ref=where, dst_ref=where,
            send_sem=line_send.at[way, block], recv_sem=line_recv.at[block, part],
            device_id={"seq": span + 1 - 2 * way}, device_id_type=MESH,
        )

    def tree_copy(bit, kind, turn, block, part, source):
        return pltpu.make_async_remote_copy(
            src_ref=source, dst_ref=cols_ref.at[col_chunk(lane, block, part)],
            send_sem=tree_send.at[bit, kind, turn, block], recv_sem=tree_recv.at[block, part],
            device_id={"head": flip(bit)}, device_id_type=MESH,
        )

    def lane_copy(step, of_lane, block, part, source):
        return pltpu.make_async_remote_copy(
            src_ref=source, dst_ref=cols_ref.at[col_chunk(of_lane, block, part)],
            send_sem=lane_send.at[step - 1, block],
            recv_sem=lane_recv.at[step - 1, block],
            device_id={"head": mate(step)}, device_id_type=MESH,
        )

    pairs = chunks // 2
    farthest = jnp.maximum(span, seq_devices - 1 - span)
    tree_now = [
        [turn * above[bit] + (1 - turn) * below[bit] == 0 for bit in range(bits)]
        for turn in range(2)
    ]
    tree_depth = above[0]
    if bits == 2:
        walk_now = []
        depths = []
        for turn in range(2):
            first, last = far[turn], far[1 - turn]
            corner = first == last
            middle = jnp.logical_and(first == 1, last == 0)
            walk_now.append([corner, middle] if turn == 0 else [middle, corner])
            depths.append(first * (1 + last) + 3 * (1 - first) * last)
        lags = [
            jnp.where(depth == 1, LAG_ONE, jnp.where(depth == 2, LAG_TWO, LAG_THREE))
            for depth in depths
        ]
        tree_lag = jnp.where(tree_depth == 1, LAG_ONE, LAG_TWO)
        longest = LAG_THREE
        kinds = 2
    else:
        walk_now = tree_now
        lags = [LAG_ONE * tree_depth] * 2
        longest = LAG_ONE * bits
        kinds = 1

    def share(turn, block, part, source, kind):
        now = tree_now if kind else walk_now
        for bit in range(bits):
            @pl.when(now[turn][bit])
            def _():
                tree_copy(bit, kind, turn, block, part, source).start()
        for step in range(1, lanes):
            lane_copy(step, lane, block, part, source).start()

    def spread(turn, block, pair):
        part = 2 * pair + turn
        source = rows_ref.at[row_chunk(block, part)]
        if kinds == 2:
            final = jnp.abs(block - span) == farthest

            @pl.when(final)
            def _():
                share(turn, block, part, source, 1)

            @pl.when(jnp.logical_not(final))
            def _():
                share(turn, block, part, source, 0)
        else:
            share(turn, block, part, source, 0)

    def pass_on(block, part, up, down, held=rows_ref):
        @pl.when(up)
        def _():
            line_copy(0, block, part, held).start()

        @pl.when(down)
        def _():
            line_copy(1, block, part, held).start()

    def pair_columns(pair, base=0):
        return pl.ds(pl.multiple_of(base + pair * 2 * chunk_width, 2 * chunk_width), 2 * chunk_width)

    def on_rows(block, pair):
        rows = block_rows(block)

        @pl.when(root)
        def _():
            for turn in range(2):
                spread(turn, block, pair)
            cols_ref[rows, pair_columns(pair, lane * width)] = rows_ref[rows, pair_columns(pair)]

        turned_ref[pair_columns(pair), rows] = rows_ref[rows, pair_columns(pair)].T

    has_up = span < seq_devices - 1
    has_down = span > 0

    for part in range(2 * raw_pairs):
        pass_on(span, part, has_up, has_down, raw_ref)

    for step in range(1, SPANS):
        for copy in kv_arrivals(step):
            copy.wait_recv()

    keys = kbuf[...].reshape(SPANS * tokens, HD)
    values = vbuf[...].reshape(SPANS * tokens, HD)
    key_places = jnp.concatenate([pbuf[j] for j in range(SPANS)], axis=1)

    def attend(held, rows, start, heads, at):
        query_places = jnp.broadcast_to(pbuf[at][0:1, 0:1], (tokens, 1)) + lax.broadcasted_iota(
            jnp.int32, (tokens, 1), 0
        )
        visible = key_places <= query_places
        pieces = []
        for h in range(heads):
            queries = held[rows, pl.ds(pl.multiple_of(start + h * HD, HD), HD)]
            scores = lax.dot_general(
                queries, keys, (((1,), (1,)), ((), ())), preferred_element_type=jnp.float32
            ) * score_scale
            masked = jnp.where(visible, scores, -jnp.inf)
            row_top = jnp.max(masked, axis=1, keepdims=True)
            weights = jnp.exp(masked - row_top)
            weight_sum = jnp.sum(weights, axis=1, keepdims=True)
            mixed = jnp.dot(
                weights.astype(jnp.bfloat16), values, preferred_element_type=jnp.float32
            )
            pieces.append((mixed / weight_sum).astype(jnp.bfloat16))
        return jnp.concatenate(pieces, axis=1)

    batch = max(1, min(COMPUTE_HEADS // (2 * chunk_heads), pairs - raw_pairs))
    while pairs % batch or raw_pairs % batch:
        batch -= 1

    def compute(step, carry):
        raw_steps = raw_pairs // batch
        steps = pairs // batch
        where = step + raw_steps
        group = jnp.where(where >= steps, where - steps, where)
        start = group * (batch * 2 * chunk_width)
        joined = attend(q_ref, pl.ds(0, tokens), start, batch * 2 * chunk_heads, place)
        columns = pl.ds(pl.multiple_of(start, batch * 2 * chunk_width), batch * 2 * chunk_width)
        rows_ref[own_rows, columns] = joined
        attended_ref[:, columns] = joined
        sent = group >= raw_steps
        for which in range(batch):
            for turn in range(2):
                pass_on(
                    span, 2 * (group * batch + which) + turn,
                    jnp.logical_and(has_up, sent), jnp.logical_and(has_down, sent),
                )
        for which in range(batch):
            on_rows(span, group * batch + which)
        return carry

    lax.fori_loop(0, pairs // batch, compute, 0)

    def arrive(way, block, pair):
        up = has_up if way == 0 else False
        down = has_down if way == 1 else False

        def ready(held):
            for turn in range(2):
                line_copy(way, block, 2 * pair + turn, held).wait_recv()
                pass_on(block, 2 * pair + turn, up, down, held)

        if raw_pairs:
            @pl.when(pair >= raw_pairs)
            def _():
                ready(rows_ref)

            @pl.when(pair < raw_pairs)
            def _():
                ready(raw_ref)
                rows = block_rows(block)
                rows_ref[rows, pair_columns(pair)] = attend(
                    raw_ref, rows, pair * 2 * chunk_width, 2 * chunk_heads, lax.rem(block, SPANS)
                )
        else:
            ready(rows_ref)
        on_rows(block, pair)

    def from_parent(turn, block, pair, kind):
        part = 2 * pair + turn
        source = cols_ref.at[col_chunk(lane, block, part)]
        tree_copy(0, kind, turn, block, part, source).wait_recv()
        share(turn, block, part, source, kind)

    def at_distance(distance, known, act):
        @pl.when(jnp.logical_and(known, distance <= span))
        def _():
            act(span - distance)

        @pl.when(
            jnp.logical_and(known, jnp.logical_and(distance > 0, span + distance < seq_devices))
        )
        def _():
            act(span + distance)

    def behind(item, lag):
        late = item - LEAD - lag
        distance = lax.div(jnp.maximum(late, 0), pairs)
        pair = jnp.maximum(late, 0) - distance * pairs
        if raw_pairs:
            turned = jnp.where(pair < pairs - raw_pairs, pair + raw_pairs, pair + raw_pairs - pairs)
            pair = jnp.where(distance == 0, turned, pair)
        return distance, pair, jnp.logical_and(not_root, late >= 0)

    def walk(item):
        for turn in range(2):
            distance, pair, known = behind(item, lags[turn])
            if kinds == 2:
                known = jnp.logical_and(known, distance != farthest)
            at_distance(distance, known, lambda block: from_parent(turn, block, pair, 0))
        if kinds == 2:
            distance, pair, known = behind(item, tree_lag)

            def both(block):
                for turn in range(2):
                    from_parent(turn, block, pair, 1)

            at_distance(distance, jnp.logical_and(known, distance == farthest), both)

    def relay(item, carry):
        reach = lax.div(item, pairs)
        pair = item - reach * pairs

        @pl.when(reach <= span)
        def _():
            arrive(0, span - reach, pair)

        @pl.when(span + reach < seq_devices)
        def _():
            arrive(1, span + reach, pair)

        walk(item)
        return carry

    def late_walk(item, carry):
        walk(item)
        return carry

    lax.fori_loop(0, pairs, late_walk, 0)
    lax.fori_loop(pairs, seq_devices * pairs, relay, 0)
    lax.fori_loop(seq_devices * pairs, seq_devices * pairs + LEAD + longest, late_walk, 0)

    def sized(rows, columns, send, recv):
        view = rows_ref.at[pl.ds(0, rows), pl.ds(0, columns)]
        return pltpu.make_async_remote_copy(
            src_ref=view, dst_ref=view, send_sem=send, recv_sem=recv,
            device_id={"head": mate(1)}, device_id_type=MESH,
        )

    def drain(block, carry):
        spare = tree_recv.at[block, 0]

        @pl.when(jnp.logical_and(has_up, block <= span))
        def _():
            sized(tokens, width, line_send.at[0, block], spare).wait_send()

        @pl.when(jnp.logical_and(has_down, block >= span))
        def _():
            sized(tokens, width, line_send.at[1, block], spare).wait_send()

        final = jnp.abs(block - span) == farthest
        for bit in range(bits):
            for turn in range(2):
                def wait_tree(kind):
                    sized(
                        tokens, pairs * chunk_width, tree_send.at[bit, kind, turn, block], spare
                    ).wait_send()

                if kinds == 2:
                    @pl.when(jnp.logical_and(walk_now[turn][bit], jnp.logical_not(final)))
                    def _():
                        wait_tree(0)

                    @pl.when(jnp.logical_and(tree_now[turn][bit], final))
                    def _():
                        wait_tree(1)
                else:
                    @pl.when(walk_now[turn][bit])
                    def _():
                        wait_tree(0)
        for step in range(1, lanes):
            whole = sized(
                tokens, width, lane_send.at[step - 1, block], lane_recv.at[step - 1, block]
            )
            whole.wait_send()
            whole.wait_recv()
        return carry

    lax.fori_loop(0, seq_devices, drain, 0)

    for step in range(1, SPANS):
        for copy in kv_copies(step):
            copy.wait_send()


def hessian_kernel(own_ref, turned_ref, cols_ref, attended_ref, out_ref, ring, own_sem, ring_sem):
    tile = ring.shape[2]
    slots = ring.shape[0]
    tiles = out_ref.shape[1] // tile
    own = pltpu.make_async_copy(own_ref, attended_ref, own_sem)
    own.start()

    def columns(j):
        return pl.ds(pl.multiple_of(j * tile, tile), tile)

    rows = out_ref.shape[0] // PIECES

    def put(j, piece):
        slot = j % slots
        where = pl.ds(piece * rows, rows)
        return pltpu.make_async_copy(
            ring.at[slot, where], out_ref.at[where, columns(j)], ring_sem.at[slot, piece]
        )

    def body(j, carry):
        @pl.when(j >= slots)
        def _():
            for piece in range(PIECES):
                put(j - slots, piece).wait()

        block = cols_ref[:, columns(j)]
        for piece in range(PIECES):
            where = pl.ds(piece * rows, rows)
            ring[j % slots, where] = jnp.dot(
                turned_ref[where, :], block, preferred_element_type=jnp.float32
            )
            put(j, piece).start()
        return carry

    lax.fori_loop(0, tiles, body, 0)
    for j in range(max(0, tiles - slots), tiles):
        for piece in range(PIECES):
            put(j, piece).wait()
    own.wait()


def on_device(query_rows, key_rows, value_rows, positions):
    tokens, width = query_rows.shape
    seq_devices = lax.axis_size("seq")
    head_devices = lax.axis_size("head")
    lanes = head_devices // seq_devices
    bits = seq_devices.bit_length() - 1
    chunks = max(2, width // (CHUNK_HEADS * HD))
    raw_pairs = min(RAW_PAIRS, chunks // 2 - 1) if seq_devices == SPANS else 0
    vmem = pl.BlockSpec(memory_space=pltpu.VMEM)
    arguments = [
        pltpu.with_memory_space_constraint(array, pltpu.HBM)
        for array in (query_rows, key_rows, value_rows, positions.reshape(1, tokens))
    ]
    dma = pltpu.SemaphoreType.DMA
    own, turned, cols = pl.pallas_call(
        functools.partial(exchange_kernel, seq_devices, head_devices, chunks, raw_pairs),
        out_shape=(
            jax.ShapeDtypeStruct((tokens, width), jnp.bfloat16),
            jax.ShapeDtypeStruct((width, seq_devices * tokens), jnp.bfloat16),
            jax.ShapeDtypeStruct((seq_devices * tokens, lanes * width), jnp.bfloat16),
        ),
        in_specs=[pl.BlockSpec(memory_space=pltpu.HBM)] * 4,
        out_specs=(vmem, vmem, vmem),
        scratch_shapes=[
            pltpu.VMEM((tokens, width), jnp.bfloat16),
            pltpu.VMEM(
                (seq_devices * tokens, max(1, 2 * raw_pairs) * width // chunks), jnp.bfloat16
            ),
            pltpu.VMEM((seq_devices * tokens, width), jnp.bfloat16),
            pltpu.VMEM((SPANS, tokens, HD), jnp.bfloat16),
            pltpu.VMEM((SPANS, tokens, HD), jnp.bfloat16),
            pltpu.VMEM((SPANS, 1, tokens), jnp.int32),
            dma((5,)),
            dma((3, SPANS - 1)),
            dma((3, SPANS - 1)),
            dma((2, seq_devices)),
            dma((seq_devices, chunks)),
            dma((bits, 2 if bits == 2 else 1, 2, seq_devices)),
            dma((seq_devices, chunks)),
            dma((lanes - 1, seq_devices)),
            dma((lanes - 1, seq_devices)),
        ],
        compiler_params=pltpu.CompilerParams(
            collective_id=0, has_side_effects=True, vmem_limit_bytes=VMEM_BYTES
        ),
        name="attend_exchange",
    )(*arguments)
    breadth = cols.shape[1]
    tile = min(TILE, breadth)
    slots = min(SLOTS, breadth // tile)
    attended, hessian = pl.pallas_call(
        hessian_kernel,
        out_shape=(
            jax.ShapeDtypeStruct((tokens, width), jnp.bfloat16),
            jax.ShapeDtypeStruct((width, breadth), jnp.float32),
        ),
        in_specs=[vmem] * 3,
        out_specs=(pl.BlockSpec(memory_space=pl.ANY), pl.BlockSpec(memory_space=pl.ANY)),
        scratch_shapes=[
            pltpu.VMEM((slots, width, tile), jnp.float32),
            dma,
            dma((slots, PIECES)),
        ],
        compiler_params=pltpu.CompilerParams(vmem_limit_bytes=VMEM_BYTES),
        name="hessian",
    )(own, turned, cols)
    return (attended, hessian)


def solution(mesh):
    placed = (P("seq", "head"), P("seq", None), P("seq", None), P("seq"))
    return jax.shard_map(
        on_device,
        mesh=mesh,
        in_specs=placed,
        out_specs=(P("seq", "head"), P("head", "seq")),
        check_vma=False,
    )
```

```python
import functools

import jax
import jax.numpy as jnp
from jax import lax
from jax.experimental import pallas as pl
from jax.experimental.pallas import tpu as pltpu
from jax.sharding import PartitionSpec as P

HEADS = 128
KVH = 8
HD = 128
SPANS = 4
CHUNK_HEADS = 2
COMPUTE_HEADS = 4
LEAD = 0
MIDDLE_LEAD = 1
LAG_ONE = 1
LAG_TWO = 3
LAG_THREE = 5
RAW_PAIRS = 1
TILE = 512
PIECES = 4
SLOTS = 4
VMEM_BYTES = 28 * 1024 * 1024
MESH = pl.DeviceIdType.MESH


def exchange_kernel(
    seq_devices, head_devices, chunks, raw_pairs,
    q_hbm, k_hbm, v_hbm, pos_hbm, attended_ref, turned_ref, cols_ref,
    q_ref, raw_ref, rows_ref, kbuf, vbuf, pbuf,
    load_sems, detour, landed, detour_load, detour_send, detour_recv, onward_send, kv_send, kv_recv, line_send, line_recv, tree_send, tree_recv, lane_send, lane_recv,
):
    tokens, width = q_ref.shape
    lanes = head_devices // seq_devices
    bits = seq_devices.bit_length() - 1
    chunk_width = width // chunks
    chunk_heads = chunk_width // HD
    raw_width = raw_pairs * 2 * chunk_width
    score_scale = HD ** (-0.5)
    head = lax.axis_index("head")
    span = lax.axis_index("seq")
    node, lane = head // lanes, head % lanes
    group = (span // SPANS) * SPANS
    place = span % SPANS

    def flip(bit):
        has = (node // 2**bit) % 2
        return (node + (1 - 2 * has) * 2**bit) * lanes + lane

    far = [(node // 2**bit + span // 2**bit) % 2 for bit in range(bits)]
    above = [sum(far[bit:]) for bit in range(bits)]
    below = [sum(far[: bit + 1]) for bit in range(bits)]
    root = above[0] == 0
    not_root = above[0] > 0

    def peer(step):
        return group + (place + step) % SPANS

    shifted = bits == 2 and seq_devices == SPANS
    ends = (0, seq_devices - 1)
    at_end = jnp.logical_or(span == 0, span == seq_devices - 1)

    def across(move):
        return head + sum(flip(bit) - head for bit in range(bits) if move // 2**bit % 2)

    def mate(step):
        return node * lanes + (lane + step) % lanes

    key_head = head * (width // HD) // (HEADS // KVH)
    key_columns = pl.ds(pl.multiple_of(key_head * HD, HD), HD)
    own_rows = pl.ds(pl.multiple_of(span * tokens, tokens), tokens)
    loads = [
        pltpu.make_async_copy(k_hbm.at[:, key_columns], kbuf.at[place], load_sems.at[0]),
        pltpu.make_async_copy(v_hbm.at[:, key_columns], vbuf.at[place], load_sems.at[1]),
        pltpu.make_async_copy(pos_hbm, pbuf.at[place], load_sems.at[2]),
        pltpu.make_async_copy(q_hbm, q_ref, load_sems.at[3]),
    ]
    if raw_pairs:
        loads.append(
            pltpu.make_async_copy(
                q_hbm.at[:, pl.ds(0, raw_width)], raw_ref.at[own_rows], load_sems.at[4]
            )
        )
    for load in loads:
        load.start()

    def end_columns(end):
        first = (end * lanes + lane) * (width // HD) // (HEADS // KVH)
        return pl.ds(pl.multiple_of(first * HD, HD), HD)

    def detour_loads(which_end):
        columns = end_columns(ends[which_end])
        return [
            pltpu.make_async_copy(
                array.at[:, columns], detour.at[which_end, which], detour_load.at[which_end, which]
            )
            for which, array in enumerate((k_hbm, v_hbm))
        ]

    def detour_copies(which_end):
        return [
            pltpu.make_async_remote_copy(
                src_ref=detour.at[which_end, which], dst_ref=landed.at[which],
                send_sem=detour_send.at[which_end, which], recv_sem=detour_recv.at[which],
                device_id={"seq": ends[which_end]}, device_id_type=MESH,
            )
            for which in range(2)
        ]

    def onward_copies():
        hops = lax.rem(span - node + seq_devices - 1, seq_devices)
        return [
            pltpu.make_async_remote_copy(
                src_ref=landed.at[which], dst_ref=buffer.at[node],
                send_sem=onward_send.at[which], recv_sem=kv_recv.at[which, hops],
                device_id={"head": span * lanes + lane}, device_id_type=MESH,
            )
            for which, buffer in enumerate((kbuf, vbuf))
        ]

    def each_end(act):
        for which_end in range(2):
            @pl.when(jnp.logical_and(root, span != ends[which_end]))
            def _():
                act(which_end)

    if shifted:
        @pl.when(root)
        def _():
            for which_end in range(2):
                for load in detour_loads(which_end):
                    load.start()

    barrier = pltpu.get_barrier_semaphore()
    count = 0
    for step in range(1, SPANS):
        pl.semaphore_signal(barrier, inc=1, device_id={"seq": peer(step)}, device_id_type=MESH)
        count += 1
    for move in (range(1, 2**bits) if shifted else [2**bit for bit in range(bits)]):
        pl.semaphore_signal(
            barrier, inc=1, device_id={"head": across(move)}, device_id_type=MESH
        )
        count += 1
    for step in range(1, lanes):
        pl.semaphore_signal(barrier, inc=1, device_id={"head": mate(step)}, device_id_type=MESH)
        count += 1
    if seq_devices > SPANS:
        @pl.when(span > 0)
        def _():
            pl.semaphore_signal(barrier, inc=1, device_id={"seq": span - 1}, device_id_type=MESH)

        @pl.when(span < seq_devices - 1)
        def _():
            pl.semaphore_signal(barrier, inc=1, device_id={"seq": span + 1}, device_id_type=MESH)

        @pl.when(span > 0)
        def _():
            pl.semaphore_wait(barrier, 1)

        @pl.when(span < seq_devices - 1)
        def _():
            pl.semaphore_wait(barrier, 1)

    for load in loads:
        load.wait()
    if shifted:
        @pl.when(root)
        def _():
            for which_end in range(2):
                for load in detour_loads(which_end):
                    load.wait()

    pl.semaphore_wait(barrier, count)

    def kv_copies(step):
        copies = []
        for which, (src, dst) in enumerate((
            (kbuf.at[place], kbuf.at[place]),
            (vbuf.at[place], vbuf.at[place]),
            (pbuf.at[place], pbuf.at[place]),
        )):
            copies.append(pltpu.make_async_remote_copy(
                src_ref=src, dst_ref=dst,
                send_sem=kv_send.at[which, step - 1], recv_sem=kv_recv.at[which, step - 1],
                device_id={"seq": peer(step)}, device_id_type=MESH,
            ))
        return copies

    def kv_arrivals(step):
        source = (place + SPANS - step) % SPANS
        copies = []
        for which, (src, dst) in enumerate((
            (kbuf.at[source], kbuf.at[source]),
            (vbuf.at[source], vbuf.at[source]),
            (pbuf.at[source], pbuf.at[source]),
        )):
            copies.append(pltpu.make_async_remote_copy(
                src_ref=src, dst_ref=dst,
                send_sem=kv_send.at[which, step - 1], recv_sem=kv_recv.at[which, step - 1],
                device_id={"seq": peer(step)}, device_id_type=MESH,
            ))
        return copies

    def each_kv(step, act):
        goal = peer(step)
        copies = kv_copies(step)
        act(copies[2])
        if shifted:
            round_about = jnp.logical_and(
                node == goal, jnp.logical_or(goal == 0, goal == seq_devices - 1)
            )

            @pl.when(jnp.logical_not(round_about))
            def _():
                act(copies[0])
                act(copies[1])
        else:
            act(copies[0])
            act(copies[1])

    for step in range(1, SPANS):
        each_kv(step, lambda copy: copy.start())
    if shifted:
        def depart(which_end):
            for copy in detour_copies(which_end):
                copy.start()

        each_end(depart)

    def row_chunk(block, part):
        return (
            pl.ds(pl.multiple_of(block * tokens, tokens), tokens),
            pl.ds(pl.multiple_of(part * chunk_width, chunk_width), chunk_width),
        )

    def col_chunk(of_lane, block, part):
        return (
            pl.ds(pl.multiple_of(block * tokens, tokens), tokens),
            pl.ds(pl.multiple_of(of_lane * width + part * chunk_width, chunk_width), chunk_width),
        )

    def block_rows(block):
        return pl.ds(pl.multiple_of(block * tokens, tokens), tokens)

    def line_copy(way, block, part, held=rows_ref):
        where = held.at[row_chunk(block, part)]
        return pltpu.make_async_remote_copy(
            src_ref=where, dst_ref=where,
            send_sem=line_send.at[way, block], recv_sem=line_recv.at[block, part],
            device_id={"seq": span + 1 - 2 * way}, device_id_type=MESH,
        )

    def tree_copy(bit, kind, turn, block, part, source):
        return pltpu.make_async_remote_copy(
            src_ref=source, dst_ref=cols_ref.at[col_chunk(lane, block, part)],
            send_sem=tree_send.at[bit, kind, turn, block], recv_sem=tree_recv.at[block, part],
            device_id={"head": flip(bit)}, device_id_type=MESH,
        )

    def lane_copy(step, of_lane, block, part, source):
        return pltpu.make_async_remote_copy(
            src_ref=source, dst_ref=cols_ref.at[col_chunk(of_lane, block, part)],
            send_sem=lane_send.at[step - 1, block],
            recv_sem=lane_recv.at[step - 1, block],
            device_id={"head": mate(step)}, device_id_type=MESH,
        )

    pairs = chunks // 2
    farthest = jnp.maximum(span, seq_devices - 1 - span)
    tree_now = [
        [turn * above[bit] + (1 - turn) * below[bit] == 0 for bit in range(bits)]
        for turn in range(2)
    ]
    tree_depth = above[0]
    if bits == 2:
        walk_now = []
        depths = []
        for turn in range(2):
            first, last = far[turn], far[1 - turn]
            corner = first == last
            middle = jnp.logical_and(first == 1, last == 0)
            walk_now.append([corner, middle] if turn == 0 else [middle, corner])
            depths.append(first * (1 + last) + 3 * (1 - first) * last)
        lags = [
            jnp.where(depth == 1, LAG_ONE, jnp.where(depth == 2, LAG_TWO, LAG_THREE))
            for depth in depths
        ]
        tree_lag = jnp.where(tree_depth == 1, LAG_ONE, LAG_TWO)
        longest = LAG_THREE
        kinds = 2
    else:
        walk_now = tree_now
        lags = [LAG_ONE * tree_depth] * 2
        longest = LAG_ONE * bits
        kinds = 1

    def share(turn, block, part, source, kind):
        now = tree_now if kind else walk_now
        for bit in range(bits):
            @pl.when(now[turn][bit])
            def _():
                tree_copy(bit, kind, turn, block, part, source).start()
        for step in range(1, lanes):
            lane_copy(step, lane, block, part, source).start()

    def spread(turn, block, pair):
        part = 2 * pair + turn
        source = rows_ref.at[row_chunk(block, part)]
        if kinds == 2:
            final = jnp.abs(block - span) == farthest

            @pl.when(final)
            def _():
                share(turn, block, part, source, 1)

            @pl.when(jnp.logical_not(final))
            def _():
                share(turn, block, part, source, 0)
        else:
            share(turn, block, part, source, 0)

    def pass_on(block, part, up, down, held=rows_ref):
        @pl.when(up)
        def _():
            line_copy(0, block, part, held).start()

        @pl.when(down)
        def _():
            line_copy(1, block, part, held).start()

    def pair_columns(pair, base=0):
        return pl.ds(pl.multiple_of(base + pair * 2 * chunk_width, 2 * chunk_width), 2 * chunk_width)

    def on_rows(block, pair, fresh):
        rows = block_rows(block)

        @pl.when(jnp.logical_and(root, fresh))
        def _():
            for turn in range(2):
                spread(turn, block, pair)

        @pl.when(root)
        def _():
            cols_ref[rows, pair_columns(pair, lane * width)] = rows_ref[rows, pair_columns(pair)]

        turned_ref[pair_columns(pair), rows] = rows_ref[rows, pair_columns(pair)].T

    has_up = span < seq_devices - 1
    has_down = span > 0

    for part in range(2 * raw_pairs):
        pass_on(span, part, has_up, has_down, raw_ref)

    for step in range(1, SPANS):
        for copy in kv_arrivals(step):
            copy.wait_recv()

    if shifted:
        @pl.when(jnp.logical_and(at_end, not_root))
        def _():
            for arrival, copy in zip(detour_copies(0), onward_copies()):
                arrival.wait_recv()
                copy.start()

    keys = kbuf[...].reshape(SPANS * tokens, HD)
    values = vbuf[...].reshape(SPANS * tokens, HD)
    key_places = jnp.concatenate([pbuf[j] for j in range(SPANS)], axis=1)

    def attend(held, rows, start, heads, at):
        query_places = jnp.broadcast_to(pbuf[at][0:1, 0:1], (tokens, 1)) + lax.broadcasted_iota(
            jnp.int32, (tokens, 1), 0
        )
        visible = key_places <= query_places
        pieces = []
        for h in range(heads):
            queries = held[rows, pl.ds(pl.multiple_of(start + h * HD, HD), HD)]
            scores = lax.dot_general(
                queries, keys, (((1,), (1,)), ((), ())), preferred_element_type=jnp.float32
            ) * score_scale
            masked = jnp.where(visible, scores, -jnp.inf)
            row_top = jnp.max(masked, axis=1, keepdims=True)
            weights = jnp.exp(masked - row_top)
            weight_sum = jnp.sum(weights, axis=1, keepdims=True)
            mixed = jnp.dot(
                weights.astype(jnp.bfloat16), values, preferred_element_type=jnp.float32
            )
            pieces.append((mixed / weight_sum).astype(jnp.bfloat16))
        return jnp.concatenate(pieces, axis=1)

    batch = max(1, min(COMPUTE_HEADS // (2 * chunk_heads), pairs - raw_pairs))
    while pairs % batch or raw_pairs % batch:
        batch -= 1

    def compute(step, carry):
        raw_steps = raw_pairs // batch
        steps = pairs // batch
        where = step + raw_steps
        group = jnp.where(where >= steps, where - steps, where)
        start = group * (batch * 2 * chunk_width)
        joined = attend(q_ref, pl.ds(0, tokens), start, batch * 2 * chunk_heads, place)
        columns = pl.ds(pl.multiple_of(start, batch * 2 * chunk_width), batch * 2 * chunk_width)
        rows_ref[own_rows, columns] = joined
        attended_ref[:, columns] = joined
        sent = group >= raw_steps
        for which in range(batch):
            for turn in range(2):
                pass_on(
                    span, 2 * (group * batch + which) + turn,
                    jnp.logical_and(has_up, sent), jnp.logical_and(has_down, sent),
                )
        for which in range(batch):
            on_rows(span, group * batch + which, True)
        return carry

    lax.fori_loop(0, pairs // batch, compute, 0)

    def forward(way, block, pair):
        up = has_up if way == 0 else False
        down = has_down if way == 1 else False

        def ready(held, final):
            for turn in range(2):
                line_copy(way, block, 2 * pair + turn, held).wait_recv()
                pass_on(block, 2 * pair + turn, up, down, held)
                if final:
                    @pl.when(root)
                    def _():
                        spread(turn, block, pair)

        if raw_pairs:
            @pl.when(pair >= raw_pairs)
            def _():
                ready(rows_ref, True)

            @pl.when(pair < raw_pairs)
            def _():
                ready(raw_ref, False)
        else:
            ready(rows_ref, True)

    def settle(block, pair):
        if raw_pairs:
            @pl.when(pair < raw_pairs)
            def _():
                rows = block_rows(block)
                rows_ref[rows, pair_columns(pair)] = attend(
                    raw_ref, rows, pair * 2 * chunk_width, 2 * chunk_heads, lax.rem(block, SPANS)
                )
        on_rows(block, pair, pair < raw_pairs)

    def from_parent(turn, block, pair, kind):
        part = 2 * pair + turn
        source = cols_ref.at[col_chunk(lane, block, part)]
        tree_copy(0, kind, turn, block, part, source).wait_recv()
        share(turn, block, part, source, kind)

    def at_distance(distance, known, act):
        @pl.when(jnp.logical_and(known, distance <= span))
        def _():
            act(span - distance)

        @pl.when(
            jnp.logical_and(known, jnp.logical_and(distance > 0, span + distance < seq_devices))
        )
        def _():
            act(span + distance)

    def behind(item, lag):
        late = item - jnp.where(at_end, LEAD, MIDDLE_LEAD) - lag
        distance = lax.div(jnp.maximum(late, 0), pairs)
        pair = jnp.maximum(late, 0) - distance * pairs
        if raw_pairs:
            turned = jnp.where(pair < pairs - raw_pairs, pair + raw_pairs, pair + raw_pairs - pairs)
            pair = jnp.where(distance == 0, turned, pair)
        return distance, pair, jnp.logical_and(not_root, late >= 0)

    def walk(item):
        for turn in range(2):
            distance, pair, known = behind(item, lags[turn])
            if kinds == 2:
                known = jnp.logical_and(known, distance != farthest)
            at_distance(distance, known, lambda block: from_parent(turn, block, pair, 0))
        if kinds == 2:
            distance, pair, known = behind(item, tree_lag)

            def both(block):
                for turn in range(2):
                    from_parent(turn, block, pair, 1)

            at_distance(distance, jnp.logical_and(known, distance == farthest), both)

    def relay(item, carry):
        reach = lax.div(item, pairs)
        pair = item - reach * pairs

        from_low = reach <= span
        from_high = span + reach < seq_devices

        @pl.when(from_low)
        def _():
            forward(0, span - reach, pair)

        @pl.when(from_high)
        def _():
            forward(1, span + reach, pair)

        @pl.when(from_low)
        def _():
            settle(span - reach, pair)

        @pl.when(from_high)
        def _():
            settle(span + reach, pair)

        walk(item)
        return carry

    def late_walk(item, carry):
        walk(item)
        return carry

    lax.fori_loop(0, pairs, late_walk, 0)
    lax.fori_loop(pairs, seq_devices * pairs, relay, 0)
    lax.fori_loop(seq_devices * pairs, seq_devices * pairs + max(LEAD, MIDDLE_LEAD) + longest, late_walk, 0)

    def sized(rows, columns, send, recv):
        view = rows_ref.at[pl.ds(0, rows), pl.ds(0, columns)]
        return pltpu.make_async_remote_copy(
            src_ref=view, dst_ref=view, send_sem=send, recv_sem=recv,
            device_id={"head": mate(1)}, device_id_type=MESH,
        )

    def drain(block, carry):
        spare = tree_recv.at[block, 0]

        @pl.when(jnp.logical_and(has_up, block <= span))
        def _():
            sized(tokens, width, line_send.at[0, block], spare).wait_send()

        @pl.when(jnp.logical_and(has_down, block >= span))
        def _():
            sized(tokens, width, line_send.at[1, block], spare).wait_send()

        final = jnp.abs(block - span) == farthest
        for bit in range(bits):
            for turn in range(2):
                def wait_tree(kind):
                    sized(
                        tokens, pairs * chunk_width, tree_send.at[bit, kind, turn, block], spare
                    ).wait_send()

                if kinds == 2:
                    @pl.when(jnp.logical_and(walk_now[turn][bit], jnp.logical_not(final)))
                    def _():
                        wait_tree(0)

                    @pl.when(jnp.logical_and(tree_now[turn][bit], final))
                    def _():
                        wait_tree(1)
                else:
                    @pl.when(walk_now[turn][bit])
                    def _():
                        wait_tree(0)
        for step in range(1, lanes):
            whole = sized(
                tokens, width, lane_send.at[step - 1, block], lane_recv.at[step - 1, block]
            )
            whole.wait_send()
            whole.wait_recv()
        return carry

    lax.fori_loop(0, seq_devices, drain, 0)

    for step in range(1, SPANS):
        each_kv(step, lambda copy: copy.wait_send())
    if shifted:
        def departed(which_end):
            for copy in detour_copies(which_end):
                copy.wait_send()

        each_end(departed)

        @pl.when(jnp.logical_and(at_end, not_root))
        def _():
            for copy in onward_copies():
                copy.wait_send()


def hessian_kernel(own_ref, turned_ref, cols_ref, attended_ref, out_ref, ring, own_sem, ring_sem):
    tile = ring.shape[2]
    slots = ring.shape[0]
    tiles = out_ref.shape[1] // tile
    own = pltpu.make_async_copy(own_ref, attended_ref, own_sem)
    own.start()

    def columns(j):
        return pl.ds(pl.multiple_of(j * tile, tile), tile)

    rows = out_ref.shape[0] // PIECES

    def put(j, piece):
        slot = j % slots
        where = pl.ds(piece * rows, rows)
        return pltpu.make_async_copy(
            ring.at[slot, where], out_ref.at[where, columns(j)], ring_sem.at[slot, piece]
        )

    def body(j, carry):
        @pl.when(j >= slots)
        def _():
            for piece in range(PIECES):
                put(j - slots, piece).wait()

        block = cols_ref[:, columns(j)]
        for piece in range(PIECES):
            where = pl.ds(piece * rows, rows)
            ring[j % slots, where] = jnp.dot(
                turned_ref[where, :], block, preferred_element_type=jnp.float32
            )
            put(j, piece).start()
        return carry

    lax.fori_loop(0, tiles, body, 0)
    for j in range(max(0, tiles - slots), tiles):
        for piece in range(PIECES):
            put(j, piece).wait()
    own.wait()


def on_device(query_rows, key_rows, value_rows, positions):
    tokens, width = query_rows.shape
    seq_devices = lax.axis_size("seq")
    head_devices = lax.axis_size("head")
    lanes = head_devices // seq_devices
    bits = seq_devices.bit_length() - 1
    chunks = max(2, width // (CHUNK_HEADS * HD))
    raw_pairs = min(RAW_PAIRS, chunks // 2 - 1) if seq_devices == SPANS else 0
    vmem = pl.BlockSpec(memory_space=pltpu.VMEM)
    arguments = [
        pltpu.with_memory_space_constraint(array, pltpu.HBM)
        for array in (query_rows, key_rows, value_rows, positions.reshape(1, tokens))
    ]
    dma = pltpu.SemaphoreType.DMA
    own, turned, cols = pl.pallas_call(
        functools.partial(exchange_kernel, seq_devices, head_devices, chunks, raw_pairs),
        out_shape=(
            jax.ShapeDtypeStruct((tokens, width), jnp.bfloat16),
            jax.ShapeDtypeStruct((width, seq_devices * tokens), jnp.bfloat16),
            jax.ShapeDtypeStruct((seq_devices * tokens, lanes * width), jnp.bfloat16),
        ),
        in_specs=[pl.BlockSpec(memory_space=pltpu.HBM)] * 4,
        out_specs=(vmem, vmem, vmem),
        scratch_shapes=[
            pltpu.VMEM((tokens, width), jnp.bfloat16),
            pltpu.VMEM(
                (seq_devices * tokens, max(1, 2 * raw_pairs) * width // chunks), jnp.bfloat16
            ),
            pltpu.VMEM((seq_devices * tokens, width), jnp.bfloat16),
            pltpu.VMEM((SPANS, tokens, HD), jnp.bfloat16),
            pltpu.VMEM((SPANS, tokens, HD), jnp.bfloat16),
            pltpu.VMEM((SPANS, 1, tokens), jnp.int32),
            dma((5,)),
            pltpu.VMEM((2, 2, tokens, HD), jnp.bfloat16),
            pltpu.VMEM((2, tokens, HD), jnp.bfloat16),
            dma((2, 2)),
            dma((2, 2)),
            dma((2,)),
            dma((2,)),
            dma((3, SPANS - 1)),
            dma((3, SPANS - 1)),
            dma((2, seq_devices)),
            dma((seq_devices, chunks)),
            dma((bits, 2 if bits == 2 else 1, 2, seq_devices)),
            dma((seq_devices, chunks)),
            dma((lanes - 1, seq_devices)),
            dma((lanes - 1, seq_devices)),
        ],
        compiler_params=pltpu.CompilerParams(
            collective_id=0, has_side_effects=True, vmem_limit_bytes=VMEM_BYTES
        ),
        name="attend_exchange",
    )(*arguments)
    breadth = cols.shape[1]
    tile = min(TILE, breadth)
    slots = min(SLOTS, breadth // tile)
    attended, hessian = pl.pallas_call(
        hessian_kernel,
        out_shape=(
            jax.ShapeDtypeStruct((tokens, width), jnp.bfloat16),
            jax.ShapeDtypeStruct((width, breadth), jnp.float32),
        ),
        in_specs=[vmem] * 3,
        out_specs=(pl.BlockSpec(memory_space=pl.ANY), pl.BlockSpec(memory_space=pl.ANY)),
        scratch_shapes=[
            pltpu.VMEM((slots, width, tile), jnp.float32),
            dma,
            dma((slots, PIECES)),
        ],
        compiler_params=pltpu.CompilerParams(vmem_limit_bytes=VMEM_BYTES),
        name="hessian",
    )(own, turned, cols)
    return (attended, hessian)


def solution(mesh):
    placed = (P("seq", "head"), P("seq", None), P("seq", None), P("seq"))
    return jax.shard_map(
        on_device,
        mesh=mesh,
        in_specs=placed,
        out_specs=(P("seq", "head"), P("head", "seq")),
        check_vma=False,
    )
```

```python
import functools

import jax
import jax.numpy as jnp
from jax import lax
from jax.experimental import pallas as pl
from jax.experimental.pallas import tpu as pltpu
from jax.sharding import PartitionSpec as P

HEADS = 128
KVH = 8
HD = 128
SPANS = 4
CHUNK_HEADS = 2
COMPUTE_HEADS = 4
LEAD = 0
MIDDLE_LEAD = 1
LAG_ONE = 1
LAG_TWO = 3
LAG_THREE = 6
RAW_PAIRS = 2
TILE = 512
PIECES = 4
SLOTS = 4
VMEM_BYTES = 28 * 1024 * 1024
MESH = pl.DeviceIdType.MESH


def exchange_kernel(
    seq_devices, head_devices, chunks, raw_pairs,
    q_hbm, k_hbm, v_hbm, pos_hbm, attended_ref, turned_ref, cols_ref,
    q_ref, raw_ref, rows_ref, kbuf, vbuf, pbuf,
    load_sems, detour, landed, detour_load, detour_send, detour_recv, onward_send, kv_send, kv_recv, line_send, line_recv, tree_send, tree_recv, corner_send, lane_send, lane_recv,
):
    tokens, width = q_ref.shape
    lanes = head_devices // seq_devices
    bits = seq_devices.bit_length() - 1
    chunk_width = width // chunks
    chunk_heads = chunk_width // HD
    raw_width = raw_pairs * 2 * chunk_width
    score_scale = HD ** (-0.5)
    head = lax.axis_index("head")
    span = lax.axis_index("seq")
    node, lane = head // lanes, head % lanes
    group = (span // SPANS) * SPANS
    place = span % SPANS

    def flip(bit):
        has = (node // 2**bit) % 2
        return (node + (1 - 2 * has) * 2**bit) * lanes + lane

    far = [(node // 2**bit + span // 2**bit) % 2 for bit in range(bits)]
    above = [sum(far[bit:]) for bit in range(bits)]
    below = [sum(far[: bit + 1]) for bit in range(bits)]
    root = above[0] == 0
    not_root = above[0] > 0

    def peer(step):
        return group + (place + step) % SPANS

    shifted = bits == 2 and seq_devices == SPANS
    ends = (0, seq_devices - 1)
    at_end = jnp.logical_or(span == 0, span == seq_devices - 1)

    def across(move):
        return head + sum(flip(bit) - head for bit in range(bits) if move // 2**bit % 2)

    def mate(step):
        return node * lanes + (lane + step) % lanes

    key_head = head * (width // HD) // (HEADS // KVH)
    key_columns = pl.ds(pl.multiple_of(key_head * HD, HD), HD)
    own_rows = pl.ds(pl.multiple_of(span * tokens, tokens), tokens)
    loads = [
        pltpu.make_async_copy(k_hbm.at[:, key_columns], kbuf.at[place], load_sems.at[0]),
        pltpu.make_async_copy(v_hbm.at[:, key_columns], vbuf.at[place], load_sems.at[1]),
        pltpu.make_async_copy(pos_hbm, pbuf.at[place], load_sems.at[2]),
        pltpu.make_async_copy(q_hbm, q_ref, load_sems.at[3]),
    ]
    if raw_pairs:
        loads.append(
            pltpu.make_async_copy(
                q_hbm.at[:, pl.ds(0, raw_width)], raw_ref.at[own_rows], load_sems.at[4]
            )
        )
    for load in loads:
        load.start()

    def end_columns(end):
        first = (end * lanes + lane) * (width // HD) // (HEADS // KVH)
        return pl.ds(pl.multiple_of(first * HD, HD), HD)

    def detour_loads(which_end):
        columns = end_columns(ends[which_end])
        return [
            pltpu.make_async_copy(
                array.at[:, columns], detour.at[which_end, which], detour_load.at[which_end, which]
            )
            for which, array in enumerate((k_hbm, v_hbm))
        ]

    def detour_copies(which_end):
        return [
            pltpu.make_async_remote_copy(
                src_ref=detour.at[which_end, which], dst_ref=landed.at[which],
                send_sem=detour_send.at[which_end, which], recv_sem=detour_recv.at[which],
                device_id={"seq": ends[which_end]}, device_id_type=MESH,
            )
            for which in range(2)
        ]

    def onward_copies():
        hops = lax.rem(span - node + seq_devices - 1, seq_devices)
        return [
            pltpu.make_async_remote_copy(
                src_ref=landed.at[which], dst_ref=buffer.at[node],
                send_sem=onward_send.at[which], recv_sem=kv_recv.at[which, hops],
                device_id={"head": span * lanes + lane}, device_id_type=MESH,
            )
            for which, buffer in enumerate((kbuf, vbuf))
        ]

    def each_end(act):
        for which_end in range(2):
            @pl.when(jnp.logical_and(root, span != ends[which_end]))
            def _():
                act(which_end)

    if shifted:
        @pl.when(root)
        def _():
            for which_end in range(2):
                for load in detour_loads(which_end):
                    load.start()

    barrier = pltpu.get_barrier_semaphore()
    count = 0
    for step in range(1, SPANS):
        pl.semaphore_signal(barrier, inc=1, device_id={"seq": peer(step)}, device_id_type=MESH)
        count += 1
    for move in (range(1, 2**bits) if shifted else [2**bit for bit in range(bits)]):
        pl.semaphore_signal(
            barrier, inc=1, device_id={"head": across(move)}, device_id_type=MESH
        )
        count += 1
    for step in range(1, lanes):
        pl.semaphore_signal(barrier, inc=1, device_id={"head": mate(step)}, device_id_type=MESH)
        count += 1
    if seq_devices > SPANS:
        @pl.when(span > 0)
        def _():
            pl.semaphore_signal(barrier, inc=1, device_id={"seq": span - 1}, device_id_type=MESH)

        @pl.when(span < seq_devices - 1)
        def _():
            pl.semaphore_signal(barrier, inc=1, device_id={"seq": span + 1}, device_id_type=MESH)

        @pl.when(span > 0)
        def _():
            pl.semaphore_wait(barrier, 1)

        @pl.when(span < seq_devices - 1)
        def _():
            pl.semaphore_wait(barrier, 1)

    for load in loads:
        load.wait()
    if shifted:
        @pl.when(root)
        def _():
            for which_end in range(2):
                for load in detour_loads(which_end):
                    load.wait()

    pl.semaphore_wait(barrier, count)

    def kv_copies(step):
        copies = []
        for which, (src, dst) in enumerate((
            (kbuf.at[place], kbuf.at[place]),
            (vbuf.at[place], vbuf.at[place]),
            (pbuf.at[place], pbuf.at[place]),
        )):
            copies.append(pltpu.make_async_remote_copy(
                src_ref=src, dst_ref=dst,
                send_sem=kv_send.at[which, step - 1], recv_sem=kv_recv.at[which, step - 1],
                device_id={"seq": peer(step)}, device_id_type=MESH,
            ))
        return copies

    def kv_arrivals(step):
        source = (place + SPANS - step) % SPANS
        copies = []
        for which, (src, dst) in enumerate((
            (kbuf.at[source], kbuf.at[source]),
            (vbuf.at[source], vbuf.at[source]),
            (pbuf.at[source], pbuf.at[source]),
        )):
            copies.append(pltpu.make_async_remote_copy(
                src_ref=src, dst_ref=dst,
                send_sem=kv_send.at[which, step - 1], recv_sem=kv_recv.at[which, step - 1],
                device_id={"seq": peer(step)}, device_id_type=MESH,
            ))
        return copies

    def each_kv(step, act):
        goal = peer(step)
        copies = kv_copies(step)
        act(copies[2])
        if shifted:
            round_about = jnp.logical_and(
                node == goal, jnp.logical_or(goal == 0, goal == seq_devices - 1)
            )

            @pl.when(jnp.logical_not(round_about))
            def _():
                act(copies[0])
                act(copies[1])
        else:
            act(copies[0])
            act(copies[1])

    for step in range(1, SPANS):
        each_kv(step, lambda copy: copy.start())
    if shifted:
        def depart(which_end):
            for copy in detour_copies(which_end):
                copy.start()

        each_end(depart)

    def row_chunk(block, part):
        return (
            pl.ds(pl.multiple_of(block * tokens, tokens), tokens),
            pl.ds(pl.multiple_of(part * chunk_width, chunk_width), chunk_width),
        )

    def col_chunk(of_lane, block, part):
        return (
            pl.ds(pl.multiple_of(block * tokens, tokens), tokens),
            pl.ds(pl.multiple_of(of_lane * width + part * chunk_width, chunk_width), chunk_width),
        )

    def block_rows(block):
        return pl.ds(pl.multiple_of(block * tokens, tokens), tokens)

    def line_copy(way, block, part, held=rows_ref):
        where = held.at[row_chunk(block, part)]
        return pltpu.make_async_remote_copy(
            src_ref=where, dst_ref=where,
            send_sem=line_send.at[way, block], recv_sem=line_recv.at[block, part],
            device_id={"seq": span + 1 - 2 * way}, device_id_type=MESH,
        )

    def tree_copy(bit, kind, turn, block, part, source):
        return pltpu.make_async_remote_copy(
            src_ref=source, dst_ref=cols_ref.at[col_chunk(lane, block, part)],
            send_sem=tree_send.at[bit, kind, turn, block], recv_sem=tree_recv.at[block, part],
            device_id={"head": flip(bit)}, device_id_type=MESH,
        )

    def corner_copy(block, source):
        return pltpu.make_async_remote_copy(
            src_ref=source, dst_ref=cols_ref.at[col_chunk(lane, block, chunks - 1)],
            send_sem=corner_send.at[block], recv_sem=tree_recv.at[block, chunks - 1],
            device_id={"head": across(2**bits - 1)}, device_id_type=MESH,
        )

    def lane_copy(step, of_lane, block, part, source):
        return pltpu.make_async_remote_copy(
            src_ref=source, dst_ref=cols_ref.at[col_chunk(of_lane, block, part)],
            send_sem=lane_send.at[step - 1, block],
            recv_sem=lane_recv.at[step - 1, block],
            device_id={"head": mate(step)}, device_id_type=MESH,
        )

    pairs = chunks // 2
    farthest = jnp.maximum(span, seq_devices - 1 - span)
    tree_now = [
        [turn * above[bit] + (1 - turn) * below[bit] == 0 for bit in range(bits)]
        for turn in range(2)
    ]
    tree_depth = above[0]
    if bits == 2:
        walk_now = []
        depths = []
        for turn in range(2):
            first, last = far[turn], far[1 - turn]
            corner = first == last
            middle = jnp.logical_and(first == 1, last == 0)
            walk_now.append([corner, middle] if turn == 0 else [middle, corner])
            depths.append(first * (1 + last) + 3 * (1 - first) * last)
        lags = [
            jnp.where(depth == 1, LAG_ONE, jnp.where(depth == 2, LAG_TWO, LAG_THREE))
            for depth in depths
        ]
        tree_lag = jnp.where(tree_depth == 1, LAG_ONE, LAG_TWO)
        kinds = 2
    else:
        walk_now = tree_now
        lags = [LAG_ONE * tree_depth] * 2
        kinds = 1

    def share(turn, block, part, source, kind):
        now = tree_now if kind else walk_now
        straight = shifted and kind == 1 and turn == 1
        for bit in range(bits):
            needed = now[turn][bit]
            if straight:
                needed = jnp.logical_and(needed, jnp.logical_or(root, part != chunks - 1))

            @pl.when(needed)
            def _():
                tree_copy(bit, kind, turn, block, part, source).start()
        if straight:
            @pl.when(jnp.logical_and(root, part == chunks - 1))
            def _():
                corner_copy(block, source).start()
        for step in range(1, lanes):
            lane_copy(step, lane, block, part, source).start()

    def spread(turn, block, pair):
        part = 2 * pair + turn
        source = rows_ref.at[row_chunk(block, part)]
        if kinds == 2:
            final = jnp.abs(block - span) == farthest

            @pl.when(final)
            def _():
                share(turn, block, part, source, 1)

            @pl.when(jnp.logical_not(final))
            def _():
                share(turn, block, part, source, 0)
        else:
            share(turn, block, part, source, 0)

    def pass_on(block, part, up, down, held=rows_ref):
        @pl.when(up)
        def _():
            line_copy(0, block, part, held).start()

        @pl.when(down)
        def _():
            line_copy(1, block, part, held).start()

    def pair_columns(pair, base=0):
        return pl.ds(pl.multiple_of(base + pair * 2 * chunk_width, 2 * chunk_width), 2 * chunk_width)

    def on_rows(block, pair, fresh):
        rows = block_rows(block)

        @pl.when(jnp.logical_and(root, fresh))
        def _():
            for turn in range(2):
                spread(turn, block, pair)

        @pl.when(root)
        def _():
            cols_ref[rows, pair_columns(pair, lane * width)] = rows_ref[rows, pair_columns(pair)]

        turned_ref[pair_columns(pair), rows] = rows_ref[rows, pair_columns(pair)].T

    has_up = span < seq_devices - 1
    has_down = span > 0

    for part in range(2 * raw_pairs):
        pass_on(span, part, has_up, has_down, raw_ref)

    for step in range(1, SPANS):
        for copy in kv_arrivals(step):
            copy.wait_recv()

    if shifted:
        @pl.when(jnp.logical_and(at_end, not_root))
        def _():
            for arrival, copy in zip(detour_copies(0), onward_copies()):
                arrival.wait_recv()
                copy.start()

    keys = kbuf[...].reshape(SPANS * tokens, HD)
    values = vbuf[...].reshape(SPANS * tokens, HD)
    key_places = jnp.concatenate([pbuf[j] for j in range(SPANS)], axis=1)

    def attend(held, rows, start, heads, at):
        query_places = jnp.broadcast_to(pbuf[at][0:1, 0:1], (tokens, 1)) + lax.broadcasted_iota(
            jnp.int32, (tokens, 1), 0
        )
        visible = key_places <= query_places
        pieces = []
        for h in range(heads):
            queries = held[rows, pl.ds(pl.multiple_of(start + h * HD, HD), HD)]
            scores = lax.dot_general(
                queries, keys, (((1,), (1,)), ((), ())), preferred_element_type=jnp.float32
            ) * score_scale
            masked = jnp.where(visible, scores, -jnp.inf)
            row_top = jnp.max(masked, axis=1, keepdims=True)
            weights = jnp.exp(masked - row_top)
            weight_sum = jnp.sum(weights, axis=1, keepdims=True)
            mixed = jnp.dot(
                weights.astype(jnp.bfloat16), values, preferred_element_type=jnp.float32
            )
            pieces.append((mixed / weight_sum).astype(jnp.bfloat16))
        return jnp.concatenate(pieces, axis=1)

    batch = max(1, min(COMPUTE_HEADS // (2 * chunk_heads), pairs - raw_pairs))
    while pairs % batch or raw_pairs % batch:
        batch -= 1

    def compute(step, carry):
        raw_steps = raw_pairs // batch
        steps = pairs // batch
        where = step + raw_steps
        group = jnp.where(where >= steps, where - steps, where)
        start = group * (batch * 2 * chunk_width)
        joined = attend(q_ref, pl.ds(0, tokens), start, batch * 2 * chunk_heads, place)
        columns = pl.ds(pl.multiple_of(start, batch * 2 * chunk_width), batch * 2 * chunk_width)
        rows_ref[own_rows, columns] = joined
        attended_ref[:, columns] = joined
        sent = group >= raw_steps
        for which in range(batch):
            for turn in range(2):
                pass_on(
                    span, 2 * (group * batch + which) + turn,
                    jnp.logical_and(has_up, sent), jnp.logical_and(has_down, sent),
                )
        for which in range(batch):
            on_rows(span, group * batch + which, True)
        return carry

    lax.fori_loop(0, pairs // batch, compute, 0)

    def forward(way, block, pair):
        up = has_up if way == 0 else False
        down = has_down if way == 1 else False

        def ready(held, final):
            for turn in range(2):
                line_copy(way, block, 2 * pair + turn, held).wait_recv()
                pass_on(block, 2 * pair + turn, up, down, held)
                if final:
                    @pl.when(root)
                    def _():
                        spread(turn, block, pair)

        if raw_pairs:
            @pl.when(pair >= raw_pairs)
            def _():
                ready(rows_ref, True)

            @pl.when(pair < raw_pairs)
            def _():
                ready(raw_ref, False)
        else:
            ready(rows_ref, True)

    def settle(block, pair):
        if raw_pairs:
            @pl.when(pair < raw_pairs)
            def _():
                rows = block_rows(block)
                rows_ref[rows, pair_columns(pair)] = attend(
                    raw_ref, rows, pair * 2 * chunk_width, 2 * chunk_heads, lax.rem(block, SPANS)
                )
        on_rows(block, pair, pair < raw_pairs)

    def from_parent(turn, block, pair, kind):
        part = 2 * pair + turn
        source = cols_ref.at[col_chunk(lane, block, part)]
        tree_copy(0, kind, turn, block, part, source).wait_recv()
        share(turn, block, part, source, kind)

    def at_distance(distance, known, act):
        @pl.when(jnp.logical_and(known, distance <= span))
        def _():
            act(span - distance)

        @pl.when(
            jnp.logical_and(known, jnp.logical_and(distance > 0, span + distance < seq_devices))
        )
        def _():
            act(span + distance)

    lead = jnp.where(at_end, LEAD, MIDDLE_LEAD)

    def behind(item, lag):
        late = item - lead - lag
        distance = lax.div(jnp.maximum(late, 0), pairs)
        pair = jnp.maximum(late, 0) - distance * pairs
        if raw_pairs:
            turned = jnp.where(pair < pairs - raw_pairs, pair + raw_pairs, pair + raw_pairs - pairs)
            pair = jnp.where(distance == 0, turned, pair)
        return distance, pair, jnp.logical_and(not_root, late >= 0)

    def walk(item):
        for turn in range(2):
            distance, pair, known = behind(item, lags[turn])
            if kinds == 2:
                known = jnp.logical_and(known, distance != farthest)
            at_distance(distance, known, lambda block: from_parent(turn, block, pair, 0))
        if kinds == 2:
            distance, pair, known = behind(item, tree_lag)

            def both(block):
                for turn in range(2):
                    from_parent(turn, block, pair, 1)

            at_distance(distance, jnp.logical_and(known, distance == farthest), both)

    def relay(item, carry):
        reach = lax.div(item, pairs)
        pair = item - reach * pairs

        from_low = reach <= span
        from_high = span + reach < seq_devices

        @pl.when(from_low)
        def _():
            forward(0, span - reach, pair)

        @pl.when(from_high)
        def _():
            forward(1, span + reach, pair)

        @pl.when(from_low)
        def _():
            settle(span - reach, pair)

        @pl.when(from_high)
        def _():
            settle(span + reach, pair)

        walk(item)
        return carry

    def late_walk(item, carry):
        walk(item)
        return carry

    total = seq_devices * pairs
    longest = jnp.maximum(lags[0], lags[1])
    if kinds == 2:
        final_lag = jnp.maximum(tree_lag, longest - pairs)
        first_lag = jnp.minimum(lags[0], lags[1])
    else:
        final_lag = longest
        first_lag = longest
    begin = jnp.where(root, pairs, jnp.minimum(lead + first_lag, pairs))
    trailing = jnp.where(root, 0, lead + final_lag)
    lax.fori_loop(begin, pairs, late_walk, 0)
    lax.fori_loop(pairs, total, relay, 0)
    lax.fori_loop(total, total + trailing, late_walk, 0)

    def sized(rows, columns, send, recv):
        view = rows_ref.at[pl.ds(0, rows), pl.ds(0, columns)]
        return pltpu.make_async_remote_copy(
            src_ref=view, dst_ref=view, send_sem=send, recv_sem=recv,
            device_id={"head": mate(1)}, device_id_type=MESH,
        )

    def drain(block, carry):
        spare = tree_recv.at[block, 0]

        @pl.when(jnp.logical_and(has_up, block <= span))
        def _():
            sized(tokens, width, line_send.at[0, block], spare).wait_send()

        @pl.when(jnp.logical_and(has_down, block >= span))
        def _():
            sized(tokens, width, line_send.at[1, block], spare).wait_send()

        final = jnp.abs(block - span) == farthest
        for bit in range(bits):
            for turn in range(2):
                def wait_tree(kind, count=pairs):
                    sized(
                        tokens, count * chunk_width, tree_send.at[bit, kind, turn, block], spare
                    ).wait_send()

                if kinds == 2:
                    @pl.when(jnp.logical_and(walk_now[turn][bit], jnp.logical_not(final)))
                    def _():
                        wait_tree(0)

                    relays = tree_now[turn][bit]
                    if shifted and turn == 1:
                        if pairs > 1:
                            @pl.when(jnp.logical_and(jnp.logical_and(relays, final), not_root))
                            def _():
                                wait_tree(1, pairs - 1)

                        relays = jnp.logical_and(relays, root)

                    @pl.when(jnp.logical_and(relays, final))
                    def _():
                        wait_tree(1)
                else:
                    @pl.when(walk_now[turn][bit])
                    def _():
                        wait_tree(0)
        if shifted:
            @pl.when(jnp.logical_and(root, final))
            def _():
                sized(tokens, chunk_width, corner_send.at[block], spare).wait_send()

        for step in range(1, lanes):
            whole = sized(
                tokens, width, lane_send.at[step - 1, block], lane_recv.at[step - 1, block]
            )
            whole.wait_send()
            whole.wait_recv()
        return carry

    lax.fori_loop(0, seq_devices, drain, 0)

    for step in range(1, SPANS):
        each_kv(step, lambda copy: copy.wait_send())
    if shifted:
        def departed(which_end):
            for copy in detour_copies(which_end):
                copy.wait_send()

        each_end(departed)

        @pl.when(jnp.logical_and(at_end, not_root))
        def _():
            for copy in onward_copies():
                copy.wait_send()


def hessian_kernel(own_ref, turned_ref, cols_ref, attended_ref, out_ref, ring, own_sem, ring_sem):
    tile = ring.shape[2]
    slots = ring.shape[0]
    tiles = out_ref.shape[1] // tile
    own = pltpu.make_async_copy(own_ref, attended_ref, own_sem)
    own.start()

    def columns(j):
        return pl.ds(pl.multiple_of(j * tile, tile), tile)

    rows = out_ref.shape[0] // PIECES

    def put(j, piece):
        slot = j % slots
        where = pl.ds(piece * rows, rows)
        return pltpu.make_async_copy(
            ring.at[slot, where], out_ref.at[where, columns(j)], ring_sem.at[slot, piece]
        )

    def body(j, carry):
        @pl.when(j >= slots)
        def _():
            for piece in range(PIECES):
                put(j - slots, piece).wait()

        block = cols_ref[:, columns(j)]
        for piece in range(PIECES):
            where = pl.ds(piece * rows, rows)
            ring[j % slots, where] = jnp.dot(
                turned_ref[where, :], block, preferred_element_type=jnp.float32
            )
            put(j, piece).start()
        return carry

    lax.fori_loop(0, tiles, body, 0)
    for j in range(max(0, tiles - slots), tiles):
        for piece in range(PIECES):
            put(j, piece).wait()
    own.wait()


def on_device(query_rows, key_rows, value_rows, positions):
    tokens, width = query_rows.shape
    seq_devices = lax.axis_size("seq")
    head_devices = lax.axis_size("head")
    lanes = head_devices // seq_devices
    bits = seq_devices.bit_length() - 1
    chunks = max(2, width // (CHUNK_HEADS * HD))
    raw_pairs = min(RAW_PAIRS, chunks // 2 - 1) if seq_devices == SPANS else 0
    vmem = pl.BlockSpec(memory_space=pltpu.VMEM)
    arguments = [
        pltpu.with_memory_space_constraint(array, pltpu.HBM)
        for array in (query_rows, key_rows, value_rows, positions.reshape(1, tokens))
    ]
    dma = pltpu.SemaphoreType.DMA
    own, turned, cols = pl.pallas_call(
        functools.partial(exchange_kernel, seq_devices, head_devices, chunks, raw_pairs),
        out_shape=(
            jax.ShapeDtypeStruct((tokens, width), jnp.bfloat16),
            jax.ShapeDtypeStruct((width, seq_devices * tokens), jnp.bfloat16),
            jax.ShapeDtypeStruct((seq_devices * tokens, lanes * width), jnp.bfloat16),
        ),
        in_specs=[pl.BlockSpec(memory_space=pltpu.HBM)] * 4,
        out_specs=(vmem, vmem, vmem),
        scratch_shapes=[
            pltpu.VMEM((tokens, width), jnp.bfloat16),
            pltpu.VMEM(
                (seq_devices * tokens, max(1, 2 * raw_pairs) * width // chunks), jnp.bfloat16
            ),
            pltpu.VMEM((seq_devices * tokens, width), jnp.bfloat16),
            pltpu.VMEM((SPANS, tokens, HD), jnp.bfloat16),
            pltpu.VMEM((SPANS, tokens, HD), jnp.bfloat16),
            pltpu.VMEM((SPANS, 1, tokens), jnp.int32),
            dma((5,)),
            pltpu.VMEM((2, 2, tokens, HD), jnp.bfloat16),
            pltpu.VMEM((2, tokens, HD), jnp.bfloat16),
            dma((2, 2)),
            dma((2, 2)),
            dma((2,)),
            dma((2,)),
            dma((3, SPANS - 1)),
            dma((3, SPANS - 1)),
            dma((2, seq_devices)),
            dma((seq_devices, chunks)),
            dma((bits, 2 if bits == 2 else 1, 2, seq_devices)),
            dma((seq_devices, chunks)),
            dma((seq_devices,)),
            dma((lanes - 1, seq_devices)),
            dma((lanes - 1, seq_devices)),
        ],
        compiler_params=pltpu.CompilerParams(
            collective_id=0, has_side_effects=True, vmem_limit_bytes=VMEM_BYTES
        ),
        name="attend_exchange",
    )(*arguments)
    breadth = cols.shape[1]
    tile = min(TILE, breadth)
    slots = min(SLOTS, breadth // tile)
    attended, hessian = pl.pallas_call(
        hessian_kernel,
        out_shape=(
            jax.ShapeDtypeStruct((tokens, width), jnp.bfloat16),
            jax.ShapeDtypeStruct((width, breadth), jnp.float32),
        ),
        in_specs=[vmem] * 3,
        out_specs=(pl.BlockSpec(memory_space=pl.ANY), pl.BlockSpec(memory_space=pl.ANY)),
        scratch_shapes=[
            pltpu.VMEM((slots, width, tile), jnp.float32),
            dma,
            dma((slots, PIECES)),
        ],
        compiler_params=pltpu.CompilerParams(vmem_limit_bytes=VMEM_BYTES),
        name="hessian",
    )(own, turned, cols)
    return (attended, hessian)


def solution(mesh):
    placed = (P("seq", "head"), P("seq", None), P("seq", None), P("seq"))
    return jax.shard_map(
        on_device,
        mesh=mesh,
        in_specs=placed,
        out_specs=(P("seq", "head"), P("head", "seq")),
        check_vma=False,
    )
```
